32 devices in a mesh: gx: 2 (over y), gy: 4 (over x, core), gz: 4 (over z).
Axes of the slice: x: 2, y: 2, z: 4, core: 2. Of those that a mesh axis runs over, the one named last changes fastest.
Arguments:
- features: bfloat16 [6, 8, 32, 8, 128], P('gx', 'gy', 'gz'), may hold values from -6 to 6
- positions: float32 [6, 8, 32, 24], P('gx', 'gy', 'gz'), may hold values from 0 to 256, as said below
- grid_anchor: int32 [6, 8, 32, 24], P('gx', 'gy', 'gz'), may hold values from -1 to 254, as said below
- species: int32 [6, 8, 32, 8], P('gx', 'gy', 'gz'), may hold values from 0 to 1
- neighbours: int32 [6, 8, 32, 512], P('gx', 'gy', 'gz'), may hold values from 0 to 12287, as said below
- neighbour_count: int32 [6, 8, 32, 8], P('gx', 'gy', 'gz'), may hold values from 32 to 64
- w_self: bfloat16 [128, 128], replicated, may hold values from -0.5 to 0.5
- w_neighbour: bfloat16 [128, 128], replicated, may hold values from -0.5 to 0.5
- w_radial: bfloat16 [8, 128], replicated, may hold values from -2 to 2
- radial_rates: float32 [8], replicated, may hold values from 0.05 to 2
- w_pair1: bfloat16 [128, 128], replicated, may hold values from -0.5 to 0.5
- w_pair2: bfloat16 [128, 128], replicated, may hold values from -0.5 to 0.5
- w_vector: bfloat16 [128, 128], replicated, may hold values from -0.5 to 0.5
- w_out: bfloat16 [128, 128], replicated, may hold values from -0.5 to 0.5
- w_charge: bfloat16 [128], replicated, may hold values from -0.5 to 0.5
- species_charge: float32 [2], replicated, may hold values from -1 to 1
Outputs:
- features_out: bfloat16 [6, 8, 32, 8, 128], P('gx', 'gy', 'gz')
- site_potential: float32 [6, 8, 32, 8], P('gx', 'gy', 'gz')
The draws below stay inside these ranges and needn't reach their ends.
Inputs may be any that keep to these rules, and one draw needn't show every extreme that they name: `positions`: component d of slot s of cell (cx, cy, cz) lies in that cell: between c_d * 8 and (c_d + 1) * 8. `grid_anchor`: at the same place as in positions, the whole part of the coordinate minus 1; the coordinate lies between grid_anchor + 1 and grid_anchor + 2. `neighbours`: each entry is the index ((cx * 8 + cy) * 32 + cz) * 8 + s of an atom whose cell differs from the listing atom's cell by at most one along each dimension, periodically; never the listing atom itself.
All inputs are finite; a program needn't handle non-finite values.
Results may differ from the reference program's by a relative error of at most 0.0039.
The reference program's roundings to bfloat16 on the way count: a program that leaves them out, or rounds other values in their place, can miss the bound.
Values may be sent and summed in bfloat16 or wider, within the bound.
A program may use at most 64 MiB of HBM per device.

```python
import math
import jax
import jax.numpy as jnp
from jax import lax

C = 128
K = 8
NBR = 64
SPECIES = 2
CELL = 8
BLOCK = 128
SLOTS = 8
NCX = 6
NCY = 8
NCZ = 32
NX = 48
NY = 64
NZ = 256
SCREEN = 32


def cell_corners():
    cell_x = jnp.broadcast_to(jnp.arange(NCX, dtype=jnp.int32)[:, None, None], (NCX, NCY, NCZ))
    cell_y = jnp.broadcast_to(jnp.arange(NCY, dtype=jnp.int32)[None, :, None], (NCX, NCY, NCZ))
    cell_z = jnp.broadcast_to(jnp.arange(NCZ, dtype=jnp.int32)[None, None, :], (NCX, NCY, NCZ))
    return (jnp.stack([cell_x, cell_y, cell_z], axis=3) * CELL)[:, :, :, :, None]


def placement_parts(key):
    inner_cell = jax.random.randint(jax.random.fold_in(key, 11), (NCX, NCY, NCZ, 3, SLOTS), 0, CELL)
    return cell_corners() + inner_cell


def draw_positions(key, part):
    whole_cells = placement_parts(key)
    uniform_draw = jax.random.uniform(jax.random.fold_in(key, 12), (NCX, NCY, NCZ, 3, SLOTS), jnp.float32)
    fraction = uniform_draw
    return (whole_cells.astype(jnp.float32) + fraction).reshape(NCX, NCY, NCZ, 3 * SLOTS)


def draw_grid_anchor(key, part):
    return (placement_parts(key) - 1).reshape(NCX, NCY, NCZ, 3 * SLOTS).astype(jnp.int32)


def draw_neighbours(key, part):
    draw_shape = (NCX, NCY, NCZ, SLOTS, NBR)
    steps_x = jax.random.randint(jax.random.fold_in(key, 21), draw_shape, -1, 2)
    steps_y = jax.random.randint(jax.random.fold_in(key, 22), draw_shape, -1, 2)
    steps_z = jax.random.randint(jax.random.fold_in(key, 23), draw_shape, -1, 2)
    pick_slot = jax.random.randint(jax.random.fold_in(key, 24), draw_shape, 0, SLOTS)
    cell_x = jnp.arange(NCX, dtype=jnp.int32)[:, None, None, None, None]
    cell_y = jnp.arange(NCY, dtype=jnp.int32)[None, :, None, None, None]
    cell_z = jnp.arange(NCZ, dtype=jnp.int32)[None, None, :, None, None]
    own_slot = jnp.arange(SLOTS, dtype=jnp.int32)[None, None, None, :, None]
    self_pair = (steps_x == 0) & (steps_y == 0) & (steps_z == 0) & (pick_slot == own_slot)
    pick_slot = jnp.where(self_pair, (pick_slot + 1) % SLOTS, pick_slot)
    other_x = (cell_x + steps_x) % NCX
    other_y = (cell_y + steps_y) % NCY
    other_z = (cell_z + steps_z) % NCZ
    atom_ids = ((other_x * NCY + other_y) * NCZ + other_z) * SLOTS + pick_slot
    return atom_ids.reshape(NCX, NCY, NCZ, SLOTS * NBR).astype(jnp.int32)


def with_ends(entries, own_key, smallest, high):
    shape = entries.shape
    spot = [jax.random.randint(jax.random.fold_in(own_key, axis), (), 0, shape[axis]) for axis in range(len(shape))]
    entries = entries.at[tuple(spot)].set(smallest)
    longest = shape.index(max(shape))
    spot[longest] = (spot[longest] + 1) % shape[longest]
    return entries.at[tuple(spot)].set(high)


def levels(key, shape, shards, low, largest):
    level, own = 1.0, jax.random.fold_in(key, 6)
    for axis_at, blocks in shards:
        heights = jnp.exp(jax.random.uniform(jax.random.fold_in(own, axis_at), (blocks,), jnp.float32, low / len(shards), largest / len(shards)))
        level = level * jnp.repeat(heights, shape[axis_at] // blocks).reshape([-1 if axis == axis_at else 1 for axis in range(len(shape))])
    return level


def noise(rng, shape, scale, most, pieces=(), kind=jnp.bfloat16):
    entries = scale * jax.random.normal(rng, shape, jnp.float32)
    if pieces:
        entries = entries * levels(rng, shape, pieces, -0.22, 0.18)
    return jnp.clip(entries, -most, most).astype(kind)


def setup_inputs(seed: int = 0) -> dict:
    key_of = jax.random.split(jax.random.key(seed), 17)
    return {
        "features": noise(key_of[0], (NCX, NCY, NCZ, SLOTS, C), 1.0, 6.0, ((0, 2), (1, 4), (2, 4))),
        "positions": draw_positions(jax.random.fold_in(key_of[16], 71), 0),
        "grid_anchor": draw_grid_anchor(jax.random.fold_in(key_of[16], 71), 0),
        "species": with_ends(jax.random.randint(key_of[3], (NCX, NCY, NCZ, SLOTS), 0, SPECIES), jax.random.fold_in(key_of[3], 1), 0, SPECIES - 1).astype(jnp.int32),
        "neighbours": draw_neighbours(jax.random.fold_in(key_of[16], 71), 0),
        "neighbour_count": with_ends(jax.random.randint(key_of[5], (NCX, NCY, NCZ, SLOTS), NBR // 2, NBR + 1), jax.random.fold_in(key_of[5], 1), NBR // 2, NBR).astype(jnp.int32),
        "w_self": noise(key_of[6], (C, C), C ** -0.5, 0.5),
        "w_neighbour": noise(key_of[7], (C, C), C ** -0.5, 0.5),
        "w_radial": noise(key_of[8], (K, C), K ** -0.5, 2.0),
        "radial_rates": jnp.clip(jnp.exp(jax.random.uniform(key_of[9], (K,), jnp.float32, math.log(0.05), math.log(2.0))), 0.05, 2.0),
        "w_pair1": noise(key_of[10], (C, C), C ** -0.5, 0.5),
        "w_pair2": noise(key_of[11], (C, C), C ** -0.5, 0.5),
        "w_vector": noise(key_of[12], (C, C), C ** -0.5, 0.5),
        "w_out": noise(key_of[13], (C, C), C ** -0.5, 0.5),
        "w_charge": noise(key_of[14], (C,), C ** -0.5, 0.5),
        "species_charge": jnp.clip(jax.random.uniform(key_of[15], (SPECIES,), jnp.float32, -1.0, 1.0), -1.0, 1.0),
    }


coulomb_scale = 0.25
smearing = 1.0
highest = lax.Precision.HIGHEST

def spline_weights(fraction):
    square = fraction * fraction
    cube_part = square * fraction
    remain = 1.0 - fraction
    return jnp.stack([remain * remain * remain / 6.0, (3.0 * cube_part - 6.0 * square + 4.0) / 6.0, (-3.0 * cube_part + 3.0 * square + 3.0 * fraction + 1.0) / 6.0, cube_part / 6.0], axis=-1)

def wave_squared(mode_ids, length):
    signed_modes = jnp.where(mode_ids > length // 2, mode_ids - length, mode_ids).astype(jnp.float32)
    wavenumber = signed_modes * (2.0 * math.pi / length)
    return wavenumber * wavenumber

def spline_modulus(mode_ids, length):
    real_part = jnp.zeros(mode_ids.shape, jnp.float32)
    imag_part = jnp.zeros(mode_ids.shape, jnp.float32)
    for tap_shift, coefficient in ((0, 1.0 / 6.0), (1, 4.0 / 6.0), (2, 1.0 / 6.0)):
        angles = (mode_ids * tap_shift % length).astype(jnp.float32) * (2.0 * math.pi / length)
        real_part = real_part + coefficient * jnp.cos(angles)
        imag_part = imag_part + coefficient * jnp.sin(angles)
    return real_part * real_part + imag_part * imag_part

def green_values(mode_x, mode_y, mode_z, length_x, length_y, length_z, screen_length):
    total_sq = wave_squared(mode_x, length_x) + wave_squared(mode_y, length_y) + wave_squared(mode_z, length_z)
    moduli = spline_modulus(mode_x, length_x) * spline_modulus(mode_y, length_y) * spline_modulus(mode_z, length_z)
    kernel = coulomb_scale * 4.0 * math.pi * jnp.exp(-0.5 * smearing * smearing * total_sq) / ((total_sq + 1.0 / (screen_length * screen_length)) * moduli)
    zero_mode = (mode_x == 0) & (mode_y == 0) & (mode_z == 0)
    return jnp.where(zero_mode, 0.0, kernel)

def atom_table(values):
    cell_shape = values.shape[:3]
    slot_count = values.shape[3] // 3
    grouped = values.reshape(cell_shape + (3, slot_count))
    return jnp.moveaxis(grouped, 3, 4).reshape(-1, 3)

def atom_update(hidden_rows, own_proj, sent_rows, displace, live_slots, w_radial, radial_rates, w_pair1, w_pair2, w_vector, w_out):
    row_count, list_length, channels = sent_rows.shape
    scaled = displace / CELL
    square = lax.optimization_barrier(jnp.sum(scaled * scaled, axis=2))
    radial_basis = jnp.exp(-square[:, :, None] * radial_rates[None, None, :]).astype(jnp.bfloat16)
    radial_part = jnp.dot(radial_basis.reshape(row_count * list_length, -1), w_radial, preferred_element_type=jnp.float32)
    pre_active = own_proj[:, None, :] + sent_rows.astype(jnp.float32) + radial_part.reshape(row_count, list_length, channels)
    latent = jax.nn.silu(pre_active).astype(jnp.bfloat16).reshape(row_count * list_length, channels)
    second = jax.nn.silu(jnp.dot(latent, w_pair1, preferred_element_type=jnp.float32)).astype(jnp.bfloat16)
    third_layer = jax.nn.silu(jnp.dot(second, w_pair2, preferred_element_type=jnp.float32)).astype(jnp.bfloat16)
    vector_weights = jnp.dot(third_layer, w_vector, preferred_element_type=jnp.float32).reshape(row_count, list_length, channels)
    live_float = live_slots.astype(jnp.float32)
    message = jnp.einsum('rn,rnc->rc', live_float, third_layer.reshape(row_count, list_length, channels).astype(jnp.float32), precision=highest) / NBR
    weighted = live_float[:, :, None] * scaled
    vector = jnp.einsum('rnd,rnc->rdc', weighted, vector_weights, precision=highest) / math.sqrt(NBR)
    invariant = lax.optimization_barrier(jnp.sum(vector * vector, axis=1))
    update = (message + invariant).astype(jnp.bfloat16)
    return (hidden_rows.astype(jnp.float32) + jnp.dot(update, w_out, preferred_element_type=jnp.float32)).astype(jnp.bfloat16)

def reference(features, positions, grid_anchor, species, neighbours, neighbour_count, w_self, w_neighbour, w_radial, radial_rates, w_pair1, w_pair2, w_vector, w_out, w_charge, species_charge):
    atom_count = NCX * NCY * NCZ * SLOTS
    hidden_rows = features.reshape(atom_count, C)
    place_rows = atom_table(positions)
    anchor_rows = atom_table(grid_anchor)
    species_rows = species.reshape(atom_count)
    neighbour_rows = neighbours.reshape(atom_count, NBR)
    counts = neighbour_count.reshape(atom_count)
    own_proj = jnp.dot(hidden_rows, w_self, preferred_element_type=jnp.float32)
    sent_proj = jnp.dot(hidden_rows, w_neighbour, preferred_element_type=jnp.float32).astype(jnp.bfloat16)
    box_length = jnp.array([NCX * CELL, NCY * CELL, NCZ * CELL], jnp.float32)
    list_ids = jnp.arange(NBR, dtype=jnp.int32)

    def pair_block(block_index):
        block_start = (block_index * BLOCK).astype(jnp.int32)
        block_ids = lax.dynamic_slice_in_dim(neighbour_rows, block_start, BLOCK, 0)
        own_place = lax.dynamic_slice_in_dim(place_rows, block_start, BLOCK, 0)
        displace = place_rows[block_ids] - own_place[:, None, :]
        displace = displace - box_length * jnp.floor(displace / box_length + 0.5)
        live_slots = list_ids[None, :] < lax.dynamic_slice_in_dim(counts, block_start, BLOCK, 0)[:, None]
        return atom_update(lax.dynamic_slice_in_dim(hidden_rows, block_start, BLOCK, 0), lax.dynamic_slice_in_dim(own_proj, block_start, BLOCK, 0), sent_proj[block_ids], displace, live_slots, w_radial, radial_rates, w_pair1, w_pair2, w_vector, w_out)
    updated = lax.map(pair_block, jnp.arange(atom_count // BLOCK, dtype=jnp.int32))
    features_out = updated.reshape(NCX, NCY, NCZ, SLOTS, C)
    charge = species_charge[species_rows] + jnp.dot(hidden_rows, w_charge, preferred_element_type=jnp.float32)
    tap_weights = spline_weights(place_rows - (anchor_rows + 1).astype(jnp.float32))
    tap_ids = jnp.arange(4, dtype=jnp.int32)
    index_x = (anchor_rows[:, 0:1] + tap_ids[None, :]) % NX
    index_y = (anchor_rows[:, 1:2] + tap_ids[None, :]) % NY
    index_z = (anchor_rows[:, 2:3] + tap_ids[None, :]) % NZ
    stencil = tap_weights[:, 0, :, None, None] * tap_weights[:, 1, None, :, None] * tap_weights[:, 2, None, None, :]
    amounts = charge[:, None, None, None] * stencil
    charge_grid = jnp.zeros((NX, NY, NZ), jnp.float32).at[index_x[:, :, None, None], index_y[:, None, :, None], index_z[:, None, None, :]].add(amounts)
    spectrum = jnp.fft.fftn(charge_grid)
    green = green_values(jnp.arange(NX, dtype=jnp.int32)[:, None, None], jnp.arange(NY, dtype=jnp.int32)[None, :, None], jnp.arange(NZ, dtype=jnp.int32)[None, None, :], NX, NY, NZ, SCREEN)
    potential_grid = jnp.real(jnp.fft.ifftn(spectrum * green)).astype(jnp.float32)
    sampled = potential_grid[index_x[:, :, None, None], index_y[:, None, :, None], index_z[:, None, None, :]]
    site_potential = lax.optimization_barrier(jnp.sum(sampled * stencil, axis=(1, 2, 3))).reshape(NCX, NCY, NCZ, SLOTS)
    return (features_out, site_potential)
```

```python
import functools
import math

import jax
import jax.numpy as jnp
import numpy as np
from jax import lax
from jax.experimental import pallas as pl
from jax.experimental.pallas import tpu as pltpu
from jax.sharding import PartitionSpec as P

NBR = 64
CELL = 8
AXES = ("gx", "gy", "gz")

coulomb_scale = 0.25
smearing = 1.0
highest = lax.Precision.HIGHEST


def round_bf16(x):
    return lax.reduce_precision(x, 8, 7)


def three_pieces(x):
    hi = round_bf16(x)
    mid = round_bf16(x - hi)
    lo = round_bf16(x - hi - mid)
    return hi, mid, lo


def cast_pieces(x, count):
    pieces = []
    for _ in range(count):
        piece = x.astype(jnp.bfloat16)
        pieces.append(piece)
        x = x - piece.astype(jnp.float32)
    return pieces


def silu(v):
    half = 0.5 * v
    return half + half * jnp.tanh(half)


def pair_kernel(
    cells,
    lengths,
    code_ref,
    ext_ref,
    own_ref,
    hidden_ref,
    wr_ref,
    rates_ref,
    w1_ref,
    w2_ref,
    wv_ref,
    wo_ref,
    out_ref,
    msg_ref,
    vec_ref,
    w1t_ref,
    w2t_ref,
):
    cells_x, cells_y, cells_z = cells
    f32, bf16 = jnp.float32, jnp.bfloat16
    slots = 8
    pairs = slots * NBR
    w1t_ref[...] = w1_ref[...].astype(f32).T.astype(bf16)
    w2t_ref[...] = w2_ref[...].astype(f32).T.astype(bf16)
    wr_rows = jnp.concatenate([wr_ref[...].astype(f32), jnp.zeros((8, 128), f32)], axis=1)
    zero_half = jnp.zeros((8, 128), f32)
    lane_slot = lax.broadcasted_iota(jnp.int32, (slots, pairs), 1) // NBR
    sel = jnp.where(lane_slot == lax.broadcasted_iota(jnp.int32, (slots, pairs), 0), 1.0, 0.0)
    tail = jnp.concatenate([sel, sel, sel, jnp.zeros((8, pairs), f32)], axis=0).astype(bf16)
    row_d = lax.broadcasted_iota(jnp.int32, (8, 1), 0)
    box = jnp.where(
        row_d == 0,
        float(lengths[0]),
        jnp.where(row_d == 1, float(lengths[1]), float(lengths[2])),
    )
    box_inv = 1.0 / box
    rates = rates_ref[...]

    def one_cell(c, carry):
        cz = c % cells_z
        cxy = c // cells_z
        cy = cxy % cells_y
        cx = cxy // cells_y
        row = pl.multiple_of(cz * 8, 8)
        here = pl.multiple_of(c * 8, 8)
        parts = []
        for dx in range(3):
            for dy in range(3):
                column = (cx + dx) * (cells_y + 2) + cy + dy
                parts.append(ext_ref[column, pl.ds(row, 24), :])
        mine = ext_ref[(cx + 1) * (cells_y + 2) + cy + 1, pl.ds(row + 8, 8), 128:]
        own = own_ref[pl.ds(here, 8), :]
        own_hi, own_mid, own_lo = [p.astype(f32) for p in cast_pieces(own, 3)]
        parts.append(wr_rows)
        parts.append(jnp.concatenate([own_hi, -mine], axis=1))
        parts.append(jnp.concatenate([own_mid, zero_half], axis=1))
        parts.append(jnp.concatenate([own_lo, zero_half], axis=1))
        parts.append(jnp.zeros((8, 256), f32))
        table = jnp.concatenate(parts, axis=0)
        sent_t = table[:, :128].T.astype(bf16)
        place_t = table[:, 128:].T[:32].astype(bf16)
        code = code_ref[c]
        which = code & 255
        live = jnp.where(code < 256, 1.0, 0.0)
        hot = jnp.where(
            lax.broadcasted_iota(jnp.int32, (216, pairs), 0) == which, 1.0, 0.0
        )
        hot_main = hot[:208].astype(bf16)
        hot_last = hot[208:]
        rhs_place = jnp.concatenate(
            [
                hot_main,
                jnp.concatenate([hot_last, jnp.zeros((8, pairs), f32)], axis=0).astype(bf16),
                tail,
            ],
            axis=0,
        )
        found = jnp.dot(place_t, rhs_place, preferred_element_type=f32)
        displace = found[0:8] + found[8:16] + found[16:24]
        displace = displace - box * jnp.floor(displace * box_inv + 0.5)
        scaled = displace * (1.0 / CELL)
        square = jnp.sum(scaled * scaled, axis=0, keepdims=True)
        basis = jnp.exp(-square * rates)
        rhs = jnp.concatenate(
            [hot_main, jnp.concatenate([hot_last, basis], axis=0).astype(bf16), tail], axis=0
        )
        pre = jnp.dot(sent_t, rhs, preferred_element_type=f32)
        latent = silu(pre).astype(bf16)
        second = silu(jnp.dot(w1t_ref[...], latent, preferred_element_type=f32)).astype(bf16)
        third = silu(jnp.dot(w2t_ref[...], second, preferred_element_type=f32)).astype(bf16)
        reach = scaled * live
        pieces = [p.astype(f32) for p in cast_pieces(reach, 3)]
        rows = [sel * live]
        for d in range(3):
            for piece in pieces:
                rows.append(sel * piece[d : d + 1])
        weights = jnp.concatenate(rows, axis=0).astype(bf16)
        sums = lax.dot_general(
            weights, third, (((1,), (1,)), ((), ())), preferred_element_type=f32
        )
        msg_ref[pl.ds(here, 8), :] = sums[0:8] * (1.0 / NBR)
        for d in range(3):
            base = 8 + 24 * d
            vec_ref[d, pl.ds(here, 8), :] = (
                sums[base : base + 8] + sums[base + 8 : base + 16] + sums[base + 16 : base + 24]
            )
        return carry

    lax.fori_loop(0, cells_x * cells_y * cells_z, one_cell, 0, unroll=8)
    wv = wv_ref[...].astype(f32)
    invariant = None
    for d in range(3):
        vector = jnp.dot(
            vec_ref[d], wv, precision=highest, preferred_element_type=f32
        ) * (1.0 / math.sqrt(NBR))
        part = vector * vector
        invariant = part if invariant is None else invariant + part
    update = (msg_ref[...] + invariant).astype(bf16)
    out_ref[...] = (
        hidden_ref[...].astype(f32)
        + jnp.dot(update, wo_ref[...], preferred_element_type=f32)
    ).astype(bf16)


def spline(distance):
    outer = jnp.maximum(2.0 - distance, 0.0)
    inner = jnp.maximum(1.0 - distance, 0.0)
    return (outer * outer * outer - 4.0 * (inner * inner * inner)) * (1.0 / 6.0)


def trig_basis(length):
    r = np.arange(length)
    rows = [np.cos(2 * np.pi * ((k * r) % length) / length) for k in range(length // 2 + 1)]
    rows += [np.sin(2 * np.pi * ((k * r) % length) / length) for k in range(1, length // 2)]
    modes = np.array(list(range(length // 2 + 1)) + list(range(1, length // 2)))
    return np.stack(rows), modes


def axis_terms(modes, length):
    wave = modes * (2.0 * np.pi / length)
    turn = np.exp(2j * np.pi * modes / length)
    modulus = np.abs(1 / 6 + 4 / 6 * turn + 1 / 6 * turn * turn) ** 2
    weight = np.where((modes == 0) | (2 * modes == length), 1.0, 2.0) / length
    return wave * wave, weight / modulus


def charge_kernel(
    sizes,
    lengths,
    window,
    screen,
    planes,
    atoms_ref,
    zrow_ref,
    krow_ref,
    kx_ref,
    by_ref,
    byt_ref,
    bx_ref,
    bxt_ref,
    out_ref,
    plane_ref,
    wave_ref,
):
    devices_x, devices_y, devices_z = sizes
    length_x, length_y, length_z = lengths
    grid_y = length_y // devices_y
    f32, bf16 = jnp.float32, jnp.bfloat16
    lanes = atoms_ref.shape[-1] * devices_z

    def load(gx, gy):
        base = (gx * devices_y + gy) * devices_z
        return jnp.concatenate([atoms_ref[base + i] for i in range(devices_z)], axis=1)

    def stencils(atoms, gy):
        ids_x = lax.broadcasted_iota(jnp.int32, (length_x, lanes), 0).astype(f32)
        off_x = jnp.abs(ids_x - atoms[0:1])
        rows_x = spline(jnp.minimum(off_x, length_x - off_x))
        start = (gy * grid_y - 1).astype(f32)
        ids_y = lax.broadcasted_iota(jnp.int32, (window, lanes), 0).astype(f32)
        rows_y = spline(jnp.abs(ids_y - (atoms[1:2] - start)))
        return rows_x, rows_y

    zrow = zrow_ref[my_index(sizes)]

    def spread(gx, gy):
        atoms = load(gx, gy)
        rows_x, rows_y = stencils(atoms, gy)
        place_z = atoms[2:3]
        whole = jnp.floor(place_z)
        f = place_z - whole
        sq = f * f
        cube = sq * f
        rem = 1.0 - f
        taps = [
            rem * rem * rem * (1.0 / 6.0),
            (3.0 * cube - 6.0 * sq + 4.0) * (1.0 / 6.0),
            (-3.0 * cube + 3.0 * sq + 3.0 * f + 1.0) * (1.0 / 6.0),
            cube * (1.0 / 6.0),
        ]
        turns = zrow[:, 0:1] * (whole - 1.0)
        turns = turns - length_z * jnp.floor(turns * (1.0 / length_z))
        angle = (turns - 0.5 * length_z) * (2.0 * math.pi / length_z)
        cos_a = -jnp.cos(angle)
        sin_a = -jnp.sin(angle)
        shift_c = zrow[:, 1:2]
        shift_s = zrow[:, 2:3]
        base_c = cos_a * shift_c + sin_a * shift_s
        base_s = sin_a * shift_c - cos_a * shift_s
        even = taps[0]
        odd = 0.0
        for t in range(1, 4):
            even = even + taps[t] * zrow[:, 2 + t : 3 + t]
            odd = odd + taps[t] * zrow[:, 5 + t : 6 + t]
        wave = base_c * even - base_s * odd
        wave_ref[gx * devices_y + gy] = wave
        scaled = wave * atoms[3:4]
        left = jnp.concatenate([rows_y * scaled[j : j + 1] for j in range(planes)], axis=0)
        left_hi = left.astype(bf16)
        left_lo = (left - left_hi.astype(f32)).astype(bf16)
        x_hi = rows_x.astype(bf16)
        x_lo = (rows_x - x_hi.astype(f32)).astype(bf16)
        res = lax.dot_general(
            jnp.concatenate([left_hi, left_lo], axis=0),
            jnp.concatenate([x_hi, x_lo], axis=0),
            (((1,), (1,)), ((), ())),
            preferred_element_type=f32,
        )
        half = planes * window
        res = res[:half] + res[half:]
        return res[:, :length_x] + res[:, length_x:]

    plane_ref[...] = jnp.zeros(plane_ref.shape, f32)

    def spread_group(g, carry):
        gy = g % devices_y
        total = spread(g // devices_y, gy)
        rows = pl.ds(pl.multiple_of(gy * window, 8), window)
        for j in range(planes):
            plane_ref[j, rows, :] += total[j * window : (j + 1) * window]
        return carry

    lax.fori_loop(0, devices_x * devices_y, spread_group, 0, unroll=2)

    def hdot(a, b):
        return jnp.dot(a, b, precision=highest, preferred_element_type=f32)

    along_y = jnp.concatenate([hdot(by_ref[...], plane_ref[j]) for j in range(planes)], axis=0)
    spectrum = hdot(along_y, bxt_ref[...])
    kcol = krow_ref[...]
    filtered = []
    for j in range(planes):
        q = kcol[:, 0:1] + zrow[j : j + 1, 9:10] + kx_ref[0:1, :]
        scale = kcol[:, 1:2] * zrow[j : j + 1, 10:11] * kx_ref[1:2, :]
        green = (coulomb_scale * 4.0 * math.pi) * jnp.exp(-0.5 * smearing * smearing * q)
        green = green * scale / (q + 1.0 / (screen * screen))
        green = jnp.where(q == 0.0, 0.0, green)
        filtered.append(spectrum[j * length_y : (j + 1) * length_y] * green)
    back = hdot(jnp.concatenate(filtered, axis=0), bx_ref[...])
    for j in range(planes):
        plane_ref[j] = hdot(byt_ref[...], back[j * length_y : (j + 1) * length_y])

    def sample_group(g, carry):
        gy = g % devices_y
        rows = pl.ds(pl.multiple_of(gy * window, 8), window)
        field = jnp.concatenate([plane_ref[j, rows, :] for j in range(planes)], axis=0)
        f_hi, f_mid = [p.astype(f32) for p in cast_pieces(field, 2)]
        field3 = jnp.concatenate([f_hi, f_mid, f_hi], axis=1).astype(bf16)
        atoms = load(g // devices_y, gy)
        rows_x, rows_y = stencils(atoms, gy)
        x_hi = rows_x.astype(bf16)
        x_lo = (rows_x - x_hi.astype(f32)).astype(bf16)
        values = jnp.dot(
            field3, jnp.concatenate([x_hi, x_hi, x_lo], axis=0), preferred_element_type=f32
        )
        wave = wave_ref[g]
        mixed = values[0:window] * wave[0:1]
        for j in range(1, planes):
            mixed = mixed + values[j * window : (j + 1) * window] * wave[j : j + 1]
        line = jnp.sum(mixed * rows_y, axis=0, keepdims=True)
        count = atoms_ref.shape[-1]
        for i in range(devices_z):
            out_ref[g * devices_z + i] = line[:, i * count : (i + 1) * count]
        return carry

    lax.fori_loop(0, devices_x * devices_y, sample_group, 0, unroll=2)


def coords_of(index, sizes):
    return (
        index // (sizes[1] * sizes[2]),
        (index // sizes[2]) % sizes[1],
        index % sizes[2],
    )


def my_index(sizes):
    gx, gy, gz = (lax.axis_index(a) for a in AXES)
    return (gx * sizes[1] + gy) * sizes[2] + gz


def fused_kernel(
    sizes,
    cells,
    lengths,
    window,
    screen,
    planes,
    atoms_ref,
    rows_ref,
    code_ref,
    own_ref,
    hidden_ref,
    wr_ref,
    rates_ref,
    w1_ref,
    w2_ref,
    wv_ref,
    wo_ref,
    zrow_ref,
    krow_ref,
    kx_ref,
    by_ref,
    byt_ref,
    bx_ref,
    bxt_ref,
    out_ref,
    site_ref,
    all_ref,
    near_ref,
    ext_ref,
    plane_ref,
    wave_ref,
    part_ref,
    held_ref,
    msg_ref,
    vec_ref,
    w1t_ref,
    w2t_ref,
    asend,
    arecv,
    hsend,
    hrecv,
    psend,
    precv,
    local_sem,
):
    devices = sizes[0] * sizes[1] * sizes[2]
    here = tuple(lax.axis_index(a) for a in AXES)
    me = my_index(sizes)
    copies = []
    for shift in range(27):
        step = (shift // 9 - 1, shift // 3 % 3 - 1, shift % 3 - 1)
        if step == (0, 0, 0):
            continue
        source, target, peer = [], [], []
        for axis in range(3):
            size = cells[axis]
            if step[axis] == 0:
                source.append(pl.ds(0, size))
                target.append(pl.ds(1, size))
                peer.append(here[axis])
            elif step[axis] > 0:
                source.append(pl.ds(size - 1, 1))
                target.append(pl.ds(0, 1))
                peer.append(lax.rem(here[axis] + 1, sizes[axis]))
            else:
                source.append(pl.ds(0, 1))
                target.append(pl.ds(size + 1, 1))
                peer.append(lax.rem(here[axis] + sizes[axis] - 1, sizes[axis]))
        copy = pltpu.make_async_remote_copy(
            src_ref=rows_ref.at[tuple(source)],
            dst_ref=near_ref.at[tuple(target)],
            send_sem=hsend.at[shift],
            recv_sem=hrecv.at[shift],
            device_id=tuple(peer),
            device_id_type=pl.DeviceIdType.MESH,
        )
        copies.append(copy)

    def atom_copy(o, peer, slot):
        return pltpu.make_async_remote_copy(
            src_ref=atoms_ref,
            dst_ref=all_ref.at[slot],
            send_sem=asend.at[o],
            recv_sem=arecv.at[o],
            device_id=coords_of(peer, sizes),
            device_id_type=pl.DeviceIdType.MESH,
        )

    def start(o, carry):
        atom_copy(o, lax.rem(me + o, devices), me).start()
        return carry

    lax.fori_loop(1, devices, start, 0)
    for copy in copies:
        copy.start()
    all_ref[me] = atoms_ref[...]

    def finish(o, carry):
        origin = lax.rem(me + devices - o, devices)
        atom_copy(o, origin, origin).wait()
        return carry

    lax.fori_loop(1, devices, finish, 0)
    charge_kernel(
        sizes,
        lengths,
        window,
        screen,
        planes,
        all_ref,
        zrow_ref,
        krow_ref,
        kx_ref,
        by_ref,
        byt_ref,
        bx_ref,
        bxt_ref,
        part_ref,
        plane_ref,
        wave_ref,
    )

    def part_copy(o, peer):
        return pltpu.make_async_remote_copy(
            src_ref=part_ref.at[peer],
            dst_ref=held_ref.at[o],
            send_sem=psend.at[o],
            recv_sem=precv.at[o],
            device_id=coords_of(peer, sizes),
            device_id_type=pl.DeviceIdType.MESH,
        )

    def send(o, carry):
        part_copy(o, lax.rem(me + o, devices)).start()
        return carry

    lax.fori_loop(1, devices, send, 0)
    for copy in copies:
        copy.wait()
    cells_x, cells_y, cells_z = cells
    for x in range(cells_x + 2):
        for y in range(cells_y + 2):
            inside = 1 <= x <= cells_x and 1 <= y <= cells_y
            column = x * (cells_y + 2) + y
            if inside:
                ext_ref[column, : slots_of(near_ref)] = flat32(near_ref[x, y, 0:1])
                ext_ref[column, slots_of(near_ref) : -slots_of(near_ref)] = flat32(
                    rows_ref[x - 1, y - 1]
                )
                ext_ref[column, -slots_of(near_ref) :] = flat32(
                    near_ref[x, y, cells_z + 1 : cells_z + 2]
                )
            else:
                ext_ref[column] = flat32(near_ref[x, y])
    pair_kernel(
        cells,
        lengths,
        code_ref,
        ext_ref,
        own_ref,
        hidden_ref,
        wr_ref,
        rates_ref,
        w1_ref,
        w2_ref,
        wv_ref,
        wo_ref,
        out_ref,
        msg_ref,
        vec_ref,
        w1t_ref,
        w2t_ref,
    )

    def take(o, total):
        part_copy(o, lax.rem(me + o, devices)).wait()
        return total + held_ref[o]

    site_ref[...] = lax.fori_loop(1, devices, take, part_ref[me])


def slots_of(ref):
    return ref.shape[3]


def flat32(block):
    wide = block.astype(jnp.float32)
    return wide.reshape(wide.shape[0] * wide.shape[1], wide.shape[2])


def shards(
    features,
    positions,
    grid_anchor,
    species,
    neighbours,
    neighbour_count,
    w_self,
    w_neighbour,
    w_radial,
    radial_rates,
    w_pair1,
    w_pair2,
    w_vector,
    w_out,
    w_charge,
    species_charge,
):
    f32, bf16 = jnp.float32, jnp.bfloat16
    cells_x, cells_y, cells_z, slot_count, channels = features.shape
    cell_count = cells_x * cells_y * cells_z
    atom_count = cell_count * slot_count
    sizes = tuple(lax.axis_size(a) for a in AXES)
    devices = sizes[0] * sizes[1] * sizes[2]
    totals = (cells_x * sizes[0], cells_y * sizes[1], cells_z * sizes[2])
    lengths = tuple(t * CELL for t in totals)
    length_x, length_y, length_z = lengths
    screen = 2 * cells_y * CELL

    hidden = features.reshape(atom_count, channels)
    own = jnp.dot(hidden, w_self, preferred_element_type=f32)
    sent = jnp.dot(hidden, w_neighbour, preferred_element_type=f32).astype(bf16)
    species_rows = species.reshape(atom_count)
    kind_ids = jnp.arange(species_charge.shape[0], dtype=jnp.int32)
    base_charge = jnp.sum(
        jnp.where(species_rows[:, None] == kind_ids[None, :], species_charge[None, :], 0.0), axis=1
    )
    charge = base_charge + jnp.dot(hidden, w_charge, preferred_element_type=f32)
    place = positions.reshape(cell_count, 3, slot_count)
    place_cols = jnp.moveaxis(place, 1, 0).reshape(3, atom_count)
    atoms = jnp.concatenate([place_cols, charge[None]], axis=0)

    hi, mid, lo = three_pieces(jnp.moveaxis(place, 1, 2).reshape(atom_count, 3))
    gap = jnp.zeros((atom_count, 5), f32)
    place_rows = jnp.concatenate(
        [hi, gap, mid, gap, lo, gap, jnp.zeros((atom_count, channels - 24), f32)], axis=1
    ).astype(bf16)
    rows = jnp.concatenate([sent, place_rows], axis=1)
    rows = rows.reshape(cells_x, cells_y, cells_z, slot_count, 2 * channels)
    cells = (cells_x, cells_y, cells_z)
    vmem = pl.BlockSpec(memory_space=pltpu.VMEM)
    dma = pltpu.SemaphoreType.DMA
    listed = neighbours.reshape(cells_x, cells_y, cells_z, slot_count * NBR)
    slot_ids = listed % slot_count
    cell_ids = listed // slot_count
    steps = []
    for axis, ids in enumerate(
        (cell_ids // (totals[2] * totals[1]), cell_ids // totals[2] % totals[1], cell_ids % totals[2])
    ):
        local = lax.broadcasted_iota(jnp.int32, listed.shape, axis)
        first = lax.axis_index(AXES[axis]) * (cells_x, cells_y, cells_z)[axis]
        steps.append((ids - first - local + 1 + totals[axis]) % totals[axis])
    code = ((steps[0] * 3 + steps[1]) * 3 + steps[2]) * slot_count + slot_ids
    counts = neighbour_count.reshape(cell_count, slot_count, 1)
    dead = jnp.arange(NBR, dtype=jnp.int32)[None, None, :] >= counts
    code = code.reshape(cell_count, slot_count, NBR) + jnp.where(dead, 256, 0)
    code = code.reshape(cell_count, 1, slot_count * NBR)

    share = length_z // 2 // devices
    planes = 2 * share
    window = -(-(cells_y * CELL + 4) // 8) * 8
    all_modes = np.arange(length_z // 2)
    table_k = np.stack([all_modes, all_modes], axis=1)
    phase_c = np.stack([np.ones_like(all_modes), np.zeros_like(all_modes)], axis=1)
    table_k[0, 1] = length_z // 2
    phase_c[0, 1] = 1
    table_k = table_k.reshape(devices, planes)
    phase_c = phase_c.reshape(devices, planes).astype(np.float64)
    taps = [2 * np.pi * ((table_k * t) % length_z) / length_z for t in range(1, 4)]
    basis_x, modes_x = trig_basis(length_x)
    basis_y, modes_y = trig_basis(length_y)
    qx, sx = axis_terms(modes_x, length_x)
    qy, sy = axis_terms(modes_y, length_y)
    qz, sz = axis_terms(table_k, length_z)
    krow = np.stack([qy, sy], axis=1).astype(np.float32)
    zrow = np.stack(
        [table_k, phase_c, 1.0 - phase_c]
        + [np.cos(a) for a in taps]
        + [np.sin(a) for a in taps]
        + [qz, sz],
        axis=2,
    ).astype(np.float32)
    kx = np.stack([qx, sx]).astype(np.float32)
    grid_y = cells_y * CELL
    columns = np.concatenate(
        [(np.arange(window) + g * grid_y - 1) % length_y for g in range(sizes[1])]
    )
    by = basis_y[:, columns].astype(np.float32)
    bx = basis_x.astype(np.float32)
    updated, site_potential = pl.pallas_call(
        functools.partial(fused_kernel, sizes, cells, lengths, window, screen, planes),
        out_shape=(
            jax.ShapeDtypeStruct((atom_count, channels), bf16),
            jax.ShapeDtypeStruct((1, atom_count), f32),
        ),
        in_specs=[vmem] * 18,
        out_specs=(vmem, vmem),
        scratch_shapes=[
            pltpu.VMEM((devices,) + atoms.shape, f32),
            pltpu.VMEM(tuple(c + 2 for c in cells) + (slot_count, 2 * channels), bf16),
            pltpu.VMEM(
                ((cells_x + 2) * (cells_y + 2), (cells_z + 2) * slot_count, 2 * channels), f32
            ),
            pltpu.VMEM((planes, sizes[1] * window, length_x), f32),
            pltpu.VMEM((sizes[0] * sizes[1], planes, sizes[2] * atom_count), f32),
            pltpu.VMEM((devices, 1, atom_count), f32),
            pltpu.VMEM((devices, 1, atom_count), f32),
            pltpu.VMEM((atom_count, channels), f32),
            pltpu.VMEM((3, atom_count, channels), f32),
            pltpu.VMEM((channels, channels), bf16),
            pltpu.VMEM((channels, channels), bf16),
            dma((devices,)),
            dma((devices,)),
            dma((27,)),
            dma((27,)),
            dma((devices,)),
            dma((devices,)),
            dma((2,)),
        ],
        name="fused_layer",
        compiler_params=pltpu.CompilerParams(has_side_effects=True),
    )(
        atoms,
        rows,
        code,
        own,
        hidden,
        w_radial,
        radial_rates.reshape(-1, 1),
        w_pair1,
        w_pair2,
        w_vector,
        w_out,
        jnp.asarray(zrow),
        jnp.asarray(krow),
        jnp.asarray(kx),
        jnp.asarray(by),
        jnp.asarray(np.ascontiguousarray(by.T)),
        jnp.asarray(bx),
        jnp.asarray(np.ascontiguousarray(bx.T)),
    )
    return (
        updated.reshape(features.shape),
        site_potential.reshape(cells_x, cells_y, cells_z, slot_count),
    )


def solution(mesh):
    return jax.shard_map(
        shards,
        mesh=mesh,
        in_specs=(
            P("gx", "gy", "gz", None, None),
            P("gx", "gy", "gz", None),
            P("gx", "gy", "gz", None),
            P("gx", "gy", "gz", None),
            P("gx", "gy", "gz", None),
            P("gx", "gy", "gz", None),
            P(),
            P(),
            P(),
            P(),
            P(),
            P(),
            P(),
            P(),
            P(),
            P(),
        ),
        out_specs=(P("gx", "gy", "gz", None, None), P("gx", "gy", "gz", None)),
        check_vma=False,
    )
```

```python
import functools
import math

import jax
import jax.numpy as jnp
import numpy as np
from jax import lax
from jax.experimental import pallas as pl
from jax.experimental.pallas import tpu as pltpu
from jax.sharding import PartitionSpec as P

NBR = 64
CELL = 8
LANES = 128
STEP_CELLS = 8
FIRST_PART = 7
VMEM_BYTES = 60 * 1024 * 1024
AXES = ("gx", "gy", "gz")

coulomb_scale = 0.25
smearing = 1.0
f32, bf16, i32 = jnp.float32, jnp.bfloat16, jnp.int32


def coords_of(index, sizes):
    return (
        index // (sizes[1] * sizes[2]),
        (index // sizes[2]) % sizes[1],
        index % sizes[2],
    )


def index_of(coords, sizes):
    return (coords[0] * sizes[1] + coords[1]) * sizes[2] + coords[2]


def iota(shape, axis):
    return lax.broadcasted_iota(i32, shape, axis)


def split_by(value, size):
    if size & (size - 1) == 0:
        shift = size.bit_length() - 1
        return lax.shift_right_logical(value, shift), value & (size - 1)
    high = jnp.floor((value.astype(f32) + 0.5) * (1.0 / size)).astype(i32)
    return high, value - high * size


def two_pieces(x):
    hi = x.astype(bf16)
    return hi, (x - hi.astype(f32)).astype(bf16)


def mm(a, b):
    return jnp.dot(a, b, preferred_element_type=f32)


def mm_nt(a, b):
    return lax.dot_general(a, b, (((1,), (1,)), ((), ())), preferred_element_type=f32)


def lane_pick(table, index):
    return jnp.take_along_axis(table, index, axis=1)


def silu_of_half(half):
    return (half + half * jnp.tanh(half)).astype(bf16)


def trig_basis(length):
    r = np.arange(length)
    rows = [np.cos(2 * np.pi * ((k * r) % length) / length) for k in range(length // 2 + 1)]
    rows += [np.sin(2 * np.pi * ((k * r) % length) / length) for k in range(1, length // 2)]
    modes = np.array(list(range(length // 2 + 1)) + list(range(1, length // 2)))
    return np.stack(rows), modes


def axis_terms(modes, length):
    wave = modes * (2.0 * np.pi / length)
    turn = np.exp(2j * np.pi * modes / length)
    modulus = np.abs(1 / 6 + 4 / 6 * turn + 1 / 6 * turn * turn) ** 2
    weight = np.where((modes == 0) | (2 * modes == length), 1.0, 2.0) / length
    return wave * wave, weight / modulus


def host_pieces(table):
    table = np.ascontiguousarray(table).astype(np.float32)
    hi = table.astype(jnp.bfloat16)
    lo = (table - hi.astype(np.float32)).astype(jnp.bfloat16)
    return jnp.asarray(hi), jnp.asarray(lo)


def layer_kernel(
    sizes,
    cells,
    lengths,
    screen,
    planes,
    win_x,
    win_y,
    feat_ref,
    hidden_ref,
    pos_ref,
    kind_ref,
    nbr_ref,
    count_ref,
    ws_ref,
    wn_ref,
    wr_ref,
    rates_ref,
    w1_ref,
    w2_ref,
    wv_ref,
    wo_ref,
    wc_ref,
    kinds_ref,
    zrow_ref,
    krow_ref,
    kx_ref,
    by_h_ref,
    by_l_ref,
    byt_h_ref,
    byt_l_ref,
    bxt_h_ref,
    bxt_l_ref,
    bxq_h_ref,
    bxq_l_ref,
    out_ref,
    site_ref,
    atoms_ref,
    all_ref,
    near_ref,
    sent_ref,
    own_ref,
    which_ref,
    zlane_ref,
    column_ref,
    live_ref,
    green_ref,
    line_ref,
    mine_ref,
    basis_ref,
    reach_ref,
    ztab_ref,
    plane_ref,
    along_ref,
    field_ref,
    wave_ref,
    xs_ref,
    ys_ref,
    part_ref,
    held_ref,
    msg_ref,
    vec_ref,
    bd1_ref,
    bd2_ref,
    asend,
    arecv,
    hsend,
    hrecv,
    psend,
    precv,
):
    size_x, size_y, size_z = sizes
    cells_x, cells_y, cells_z = cells
    length_x, length_y, length_z = lengths
    devices = size_x * size_y * size_z
    slots = feat_ref.shape[3]
    channels = feat_ref.shape[4]
    cell_count = cells_x * cells_y * cells_z
    atom_count = cell_count * slots
    pairs = slots * NBR
    half_pairs = pairs // 2
    run = cells_z * slots
    wide_y = cells_y + 2
    here = tuple(lax.axis_index(a) for a in AXES)
    me = index_of(here, sizes)

    offsets = [
        (a, b, c)
        for a in range(size_x)
        for b in range(size_y)
        for c in range(size_z)
        if (a, b, c) != (0, 0, 0)
    ]
    close = [
        all(step in (0, 1, size - 1) for step, size in zip(offset, sizes)) for offset in offsets
    ]
    offsets = [o for o, c in zip(offsets, close) if c] + [o for o, c in zip(offsets, close) if not c]
    close_count = sum(close)

    def moved(offset, sign):
        return tuple(
            lax.rem(at + (step if sign > 0 else size - step), size) if step else at
            for at, step, size in zip(here, offset, sizes)
        )

    barrier = pltpu.get_barrier_semaphore()
    for offset in offsets:
        pl.semaphore_signal(
            barrier, inc=1, device_id=moved(offset, 1), device_id_type=pl.DeviceIdType.MESH
        )

    pad_rows = jnp.zeros((LANES - cell_count, 1), f32)
    kinds = kind_ref[...].astype(f32)
    turned = [
        jnp.concatenate(
            [block, jnp.zeros((LANES - cell_count, block.shape[1]), f32)], axis=0
        ).T
        for block in (pos_ref[...], kinds)
    ]
    lane8 = iota((slots, LANES), 1)
    diagonal = (lane8 % slots) == iota((slots, LANES), 0)
    per_chunk = LANES // slots
    wc_rows = jnp.broadcast_to(wc_ref[...].reshape(1, channels), (slots, channels))
    readout = mm_nt(wc_rows, hidden_ref[...])

    def lined(block, chunk):
        picked = lane_pick(block, lane8 // slots + chunk * per_chunk)
        return jnp.sum(jnp.where(diagonal, picked, 0.0), axis=0, keepdims=True)

    for chunk in range(atom_count // LANES):
        where_to = slice(chunk * LANES, (chunk + 1) * LANES)
        for d in range(3):
            atoms_ref[d : d + 1, where_to] = lined(turned[0][d * slots : (d + 1) * slots], chunk)
        kind = lined(turned[1], chunk)
        charge = readout[0:1, where_to]
        for k in range(kinds_ref.shape[0]):
            charge = charge + jnp.where(kind == float(k), kinds_ref[k], 0.0)
        atoms_ref[3:4, where_to] = charge

    def atom_copy(offset, peer, slot):
        at = index_of(offset, sizes)
        return pltpu.make_async_remote_copy(
            src_ref=atoms_ref,
            dst_ref=all_ref.at[slot],
            send_sem=asend.at[at],
            recv_sem=arecv.at[at],
            device_id=peer,
            device_id_type=pl.DeviceIdType.MESH,
        )

    def wait_atoms(some):
        for offset in some:
            origin = moved(offset, -1)
            atom_copy(offset, origin, index_of(origin, sizes)).wait()

    copies = []
    for shift in range(27):
        step = (shift // 9 - 1, shift // 3 % 3 - 1, shift % 3 - 1)
        if step == (0, 0, 0):
            continue
        source, target, peer = [], [], []
        for axis in range(3):
            size = cells[axis]
            if step[axis] == 0:
                source.append(pl.ds(0, size))
                target.append(pl.ds(1, size))
                peer.append(here[axis])
            elif step[axis] > 0:
                source.append(pl.ds(size - 1, 1))
                target.append(pl.ds(0, 1))
                peer.append(lax.rem(here[axis] + 1, sizes[axis]))
            else:
                source.append(pl.ds(0, 1))
                target.append(pl.ds(size + 1, 1))
                peer.append(lax.rem(here[axis] + sizes[axis] - 1, sizes[axis]))
        copies.append(
            pltpu.make_async_remote_copy(
                src_ref=feat_ref.at[tuple(source)],
                dst_ref=near_ref.at[tuple(target)],
                send_sem=hsend.at[shift],
                recv_sem=hrecv.at[shift],
                device_id=tuple(peer),
                device_id_type=pl.DeviceIdType.MESH,
            )
        )
    pl.semaphore_wait(barrier, devices - 1)
    for offset in offsets[:close_count]:
        atom_copy(offset, moved(offset, 1), me).start()
    for copy in copies:
        copy.start()
    for offset in offsets[close_count:]:
        atom_copy(offset, moved(offset, 1), me).start()
    all_ref[me] = atoms_ref[...]

    own = mm(hidden_ref[...], ws_ref[...]) * 0.5
    own_hi = own.astype(bf16).astype(f32)
    own_ref[0] = own_hi
    own_ref[1] = (own - own_hi).astype(bf16).astype(f32)

    no_block = jnp.zeros((channels, channels), bf16)
    for ref, target in ((w1_ref, bd1_ref), (w2_ref, bd2_ref)):
        weight = ref[...] * jnp.asarray(0.5, bf16)
        target[0:channels, 0:channels] = weight
        target[0:channels, channels:] = no_block
        target[channels:, 0:channels] = no_block
        target[channels:, channels:] = weight

    listed = nbr_ref[...]
    cell_id, slot_id = split_by(listed, slots)
    xy_id, z_id = split_by(cell_id, cells_z * size_z)
    x_id, y_id = split_by(xy_id, cells_y * size_y)
    row_xy, row_z = split_by(iota((cell_count, 1), 0), cells_z)
    row_x, row_y = split_by(row_xy, cells_y)
    steps = []
    for ids, local, axis in ((x_id, row_x, 0), (y_id, row_y, 1), (z_id, row_z, 2)):
        total = cells[axis] * sizes[axis]
        gap = ids - (local + here[axis] * cells[axis])
        gap = jnp.where(gap > 1, gap - total, gap)
        steps.append(jnp.where(gap < -1, gap + total, gap))
    which = ((steps[0] + 1) * 3 + steps[1] + 1) * (3 * slots) + (steps[2] + 1) * slots + slot_id
    which_ref[...] = which.astype(f32)
    zlane_ref[...] = ((row_z + steps[2]) * slots + slot_id) & (LANES - 1)
    column_ref[...] = (steps[0] + 1) * wide_y + row_y + 1 + steps[1]
    lane_pair = iota((slots, pairs), 1)
    sel = jnp.where(lane_pair // NBR == iota((slots, pairs), 0), 1.0, 0.0)
    limit = mm(count_ref[...].astype(f32).astype(bf16), sel.astype(bf16))
    order = (iota((1, pairs), 1) % NBR).astype(f32)
    live_ref[...] = jnp.where(order < limit, 1.0, 0.0)

    zrow = zrow_ref[me]
    kcol = krow_ref[...]
    for j in range(planes):
        q = kcol[:, 0:1] + zrow[j : j + 1, 3:4] + kx_ref[0:1, :]
        scale = kcol[:, 1:2] * zrow[j : j + 1, 4:5] * kx_ref[1:2, :]
        green = (coulomb_scale * 4.0 * math.pi) * jnp.exp(-0.5 * smearing * smearing * q)
        green = green * scale / (q + 1.0 / (screen * screen))
        green_ref[j * length_y : (j + 1) * length_y] = jnp.where(q == 0.0, 0.0, green)
    plane_ref[...] = jnp.zeros(plane_ref.shape, f32)
    for z in range(size_z):
        lane = (iota((1, LANES), 1) + (z * cells_z * CELL - 1)).astype(f32)
        turns = zrow[:, 0:1] * lane
        turns = turns - length_z * jnp.floor(turns * (1.0 / length_z))
        angle = (turns - 0.5 * length_z) * (2.0 * math.pi / length_z)
        ztab_ref[z] = -jnp.cos(angle) * zrow[:, 1:2] - jnp.sin(angle) * zrow[:, 2:3]

    wait_atoms(offsets[:close_count])

    lane4 = iota((4, LANES), 1)
    for x in range(cells_x + 2):
        for pair_y in range(wide_y // 2):
            halves = []
            for y in (2 * pair_y, 2 * pair_y + 1):
                spots, locals_ = [], []
                for at, axis in ((x, 0), (y, 1)):
                    size = cells[axis]
                    if at == 0:
                        spots.append(lax.rem(here[axis] + sizes[axis] - 1, sizes[axis]))
                        locals_.append(size - 1)
                    elif at == size + 1:
                        spots.append(lax.rem(here[axis] + 1, sizes[axis]))
                        locals_.append(0)
                    else:
                        spots.append(here[axis])
                        locals_.append(at - 1)
                column = locals_[0] * cells_y + locals_[1]
                start_lane = column * run
                block = pl.ds(start_lane // LANES * LANES, LANES)
                odd = start_lane % LANES != 0
                pieces = []
                for step_z in (0, 1, size_z - 1):
                    origin = index_of(
                        (spots[0], spots[1], lax.rem(here[2] + step_z, size_z)), sizes
                    )
                    piece = all_ref[origin, :, block]
                    if (step_z == 0) == odd:
                        piece = pltpu.roll(piece, run, 1)
                    pieces.append(piece)
                line = jnp.where(
                    lane4 < run, pieces[0], jnp.where(lane4 < run + slots, pieces[1], pieces[2])
                )
                halves.append(line)
                if 1 <= x <= cells_x and 1 <= y <= cells_y:
                    mine_ref[column] = jnp.concatenate([line, line], axis=0)
            line_ref[x * (wide_y // 2) + pair_y] = jnp.concatenate(halves, axis=0)

    sub8 = iota((slots, LANES), 0)
    row_d = iota((slots, 1), 0)
    box = jnp.where(
        row_d == 0,
        float(length_x),
        jnp.where(row_d == 1, float(length_y), float(length_z)),
    )
    box_inv = 1.0 / box
    rates = jnp.zeros((rates_ref.shape[0], 1), f32)
    for k in range(rates_ref.shape[0]):
        rates = jnp.where(iota(rates.shape, 0) == k, rates_ref[k], rates)
    sub_y = sub8 // 4

    def geometry(octet, carry):
        rows = pl.ds(pl.multiple_of(octet * 8, 8), 8)
        for r in range(8):
            place_cell(octet * 8 + r, rows, r)
        return carry

    def place_cell(c, rows, r):
        cz = lax.rem(c, cells_z)
        cxy = c // cells_z
        cx = cxy // cells_y
        for chunk in range(pairs // LANES):
            part = pl.ds(chunk * LANES, LANES)
            spot = jnp.broadcast_to(zlane_ref[rows, part][r : r + 1], (slots, LANES))
            column = jnp.broadcast_to(column_ref[rows, part][r : r + 1], (slots, LANES)) - sub_y
            live = live_ref[rows, part][r : r + 1]
            which = which_ref[rows, part][r : r + 1]
            found = jnp.zeros((slots, LANES), f32)
            for dx in range(3):
                for pair_y in range(wide_y // 2):
                    table = line_ref[(cx + dx) * (wide_y // 2) + pair_y]
                    picked = lane_pick(table, spot)
                    found = jnp.where(column == dx * wide_y + 2 * pair_y, picked, found)
            found = found + pltpu.roll(found, 4, 0)
            own_spot = cz * slots + (lane8 + chunk * LANES) // NBR
            displace = found - lane_pick(mine_ref[cxy], own_spot)
            displace = displace - box * jnp.floor(displace * box_inv + 0.5)
            scaled = jnp.where(row_d < 3, displace * (1.0 / CELL), 0.0)
            square = jnp.sum(scaled * scaled, axis=0, keepdims=True)
            basis_ref[c, :, part] = jnp.exp(-square * rates)
            reach = jnp.where(row_d == 3, 1.0, scaled) * live
            reach_ref[c, :, part] = jnp.where(row_d == 4, which, reach)

    lax.fori_loop(0, cell_count // 8, geometry, 0)

    for copy in copies:
        copy.wait()
    for x in range(cells_x + 2):
        for y in range(wide_y):
            if 1 <= x <= cells_x and 1 <= y <= cells_y:
                blocks = [
                    near_ref[x, y, 0:1],
                    feat_ref[x - 1, y - 1],
                    near_ref[x, y, cells_z + 1 :],
                ]
            else:
                blocks = [near_ref[x, y]]
            line = [b.astype(f32).reshape(b.shape[0] * slots, channels) for b in blocks]
            line = jnp.concatenate(line, axis=0).astype(bf16)
            sent_ref[x * wide_y + y] = mm(line, wn_ref[...]).astype(bf16).astype(f32) * 0.5

    hot_rows = 27 * slots
    even_rows = hot_rows // 16 * 16
    hot_ids = iota((even_rows, 1), 0).astype(f32).astype(bf16)
    last_ids = (iota((hot_rows - even_rows, 1), 0) + even_rows).astype(f32)
    wr_rows = wr_ref[...].astype(f32) * 0.5
    sel_tile = jnp.concatenate([sel, sel], axis=0).astype(bf16)
    sub_h = iota((slots, half_pairs), 0)
    slot_h = iota((slots, half_pairs), 1) // NBR
    in_low = slot_h == sub_h
    in_high = slot_h == sub_h - slots // 2

    def pair_step(step, carry):
        rows = []
        for u in range(STEP_CELLS):
            c = step * STEP_CELLS + u
            cz = lax.rem(c, cells_z)
            cxy = c // cells_z
            cy = lax.rem(cxy, cells_y)
            cx = cxy // cells_y
            at = pl.ds(pl.multiple_of(cz * slots, slots), 3 * slots)
            mine = pl.ds(pl.multiple_of(c * slots, slots), slots)
            parts = []
            for dx in range(3):
                for dy in range(3):
                    parts.append(sent_ref[(cx + dx) * wide_y + cy + dy, at, :])
            parts += [wr_rows, own_ref[0, mine, :], own_ref[1, mine, :]]
            table = jnp.concatenate(parts, axis=0).astype(bf16).T
            which = reach_ref[c, 4:5, :]
            hot = jnp.where(
                hot_ids == which.astype(bf16), jnp.asarray(1.0, bf16), jnp.asarray(0.0, bf16)
            )
            last = jnp.where(last_ids == which, 1.0, 0.0)
            tile = jnp.concatenate([last, basis_ref[c]], axis=0).astype(bf16)
            rhs = jnp.concatenate([hot, tile, sel_tile], axis=0)
            latent = silu_of_half(mm(table, rhs)).T
            rows.append(jnp.concatenate([latent[:half_pairs], latent[half_pairs:]], axis=1))
        second = silu_of_half(mm(jnp.concatenate(rows, axis=0), bd1_ref[...]))
        third = silu_of_half(mm(second, bd2_ref[...]))
        for u in range(STEP_CELLS):
            c = step * STEP_CELLS + u
            mine = pl.ds(pl.multiple_of(c * slots, slots), slots)
            weights = []
            for r in (3, 0, 1, 2):
                low = reach_ref[c, r : r + 1, 0:half_pairs]
                high = reach_ref[c, r : r + 1, half_pairs:]
                full = jnp.where(in_low, low, jnp.where(in_high, high, 0.0))
                if r == 3:
                    weights.append(full)
                else:
                    full_hi = full.astype(bf16).astype(f32)
                    weights += [full_hi, full - full_hi]
            weights = jnp.concatenate(weights, axis=0).astype(bf16)
            sums = mm(weights, third[u * half_pairs : (u + 1) * half_pairs])
            rest = []
            for r in range(7):
                block = sums[r * slots : (r + 1) * slots]
                rest.append(
                    jnp.where(row_d < slots // 2, block[:, :channels], block[:, channels:])
                )
            msg_ref[mine, :] = rest[0] * (1.0 / NBR)
            for d in range(3):
                vec_ref[d, mine, :] = rest[1 + 2 * d] + rest[2 + 2 * d]
        return carry

    first_steps = cell_count // STEP_CELLS * FIRST_PART // 16
    lax.fori_loop(0, first_steps, pair_step, 0)
    wait_atoms(offsets[close_count:])

    lanes = size_z * atom_count

    def spread(g, carry):
        gx = g // size_y
        gy = lax.rem(g, size_y)
        base = g * size_z
        atoms = jnp.concatenate([all_ref[base + i] for i in range(size_z)], axis=1)
        whole = jnp.floor(atoms)
        f = atoms - whole
        sq = f * f
        cube = sq * f
        rem = 1.0 - f
        taps = [
            rem * rem * rem * (1.0 / 6.0),
            (3.0 * cube - 6.0 * sq + 4.0) * (1.0 / 6.0),
            (-3.0 * cube + 3.0 * sq + 3.0 * f + 1.0) * (1.0 / 6.0),
            cube * (1.0 / 6.0),
        ]
        first_x = (gx * (cells_x * CELL)).astype(f32)
        first_y = (gy * (cells_y * CELL)).astype(f32)
        off_x = iota((win_x, 1), 0).astype(f32).astype(bf16) - (whole[0:1] - first_x).astype(bf16)
        x_hi = jnp.zeros((win_x, lanes), bf16)
        x_lo = jnp.zeros((win_x, lanes), bf16)
        for t in range(4):
            hit = off_x == jnp.asarray(t, bf16)
            t_hi, t_lo = two_pieces(taps[t][0:1])
            x_hi = jnp.where(hit, jnp.broadcast_to(t_hi, hit.shape), x_hi)
            x_lo = jnp.where(hit, jnp.broadcast_to(t_lo, hit.shape), x_lo)
        off_y = iota((win_y, 1), 0).astype(f32) - (whole[1:2] - first_y)
        rows_y = jnp.zeros((win_y, lanes), f32)
        for t in range(4):
            rows_y = jnp.where(off_y == float(t), taps[t][1:2], rows_y)
        waves = []
        for z in range(size_z):
            table = ztab_ref[z]
            for chunk in range(atom_count // LANES):
                part = slice(z * atom_count + chunk * LANES, z * atom_count + (chunk + 1) * LANES)
                spot = (whole[2:3, part] - float(z * cells_z * CELL)).astype(i32)
                spot = jnp.broadcast_to(spot, table.shape)
                wave = None
                for t in range(4):
                    term = lane_pick(table, spot + t) * taps[t][2:3, part]
                    wave = term if wave is None else wave + term
                waves.append(wave)
        wave = jnp.concatenate(waves, axis=1)
        wave_ref[g] = wave
        ys_ref[g] = rows_y
        rows_x = jnp.concatenate([x_hi, x_lo], axis=0)
        xs_ref[g] = rows_x
        scaled = wave * atoms[3:4]
        left = jnp.concatenate([rows_y * scaled[j : j + 1] for j in range(planes)], axis=0)
        l_hi, l_lo = two_pieces(left)
        res = mm_nt(l_hi, rows_x) + mm_nt(l_lo, rows_x)
        per_block = LANES // (2 * win_x)
        res = jnp.concatenate([res, jnp.zeros((res.shape[0], LANES - 2 * win_x), f32)], axis=1)
        res = pltpu.roll(res, lax.rem(gx, per_block) * (2 * win_x), 1)
        rows = pl.ds(pl.multiple_of(gy * win_y, 8), win_y)
        for j in range(planes):
            plane_ref[gx // per_block, j, rows, :] += res[j * win_y : (j + 1) * win_y]
        return carry

    lax.fori_loop(0, size_x * size_y, spread, 0)

    spectrum = None
    for block in range(plane_ref.shape[0]):
        for j in range(planes):
            p_hi, p_lo = two_pieces(plane_ref[block, j])
            along_ref[j * length_y : (j + 1) * length_y, :] = (
                mm(by_h_ref[...], p_hi) + mm(by_h_ref[...], p_lo) + mm(by_l_ref[...], p_hi)
            )
        a_hi, a_lo = two_pieces(along_ref[...])
        part = mm(a_hi, bxt_h_ref[block]) + mm(a_lo, bxt_h_ref[block]) + mm(a_hi, bxt_l_ref[block])
        spectrum = part if spectrum is None else spectrum + part
    s_hi, s_lo = two_pieces(spectrum * green_ref[...])
    lane_x = iota((1, LANES), 1) % (2 * win_x) < win_x
    for gx in range(size_x):
        cols = slice(gx * LANES, (gx + 1) * LANES)
        back = mm(s_hi, bxq_h_ref[:, cols]) + mm(s_lo, bxq_h_ref[:, cols]) + mm(s_hi, bxq_l_ref[:, cols])
        b_hi, b_lo = two_pieces(back)
        for j in range(planes):
            rows = slice(j * length_y, (j + 1) * length_y)
            value = (
                mm(byt_h_ref[...], b_hi[rows])
                + mm(byt_h_ref[...], b_lo[rows])
                + mm(byt_l_ref[...], b_hi[rows])
            )
            v_hi = value.astype(bf16).astype(f32)
            field_ref[gx, j] = jnp.where(lane_x, v_hi, value - v_hi)

    def part_copy(o, peer):
        return pltpu.make_async_remote_copy(
            src_ref=part_ref.at[peer],
            dst_ref=held_ref.at[o],
            send_sem=psend.at[o],
            recv_sem=precv.at[o],
            device_id=coords_of(peer, sizes),
            device_id_type=pl.DeviceIdType.MESH,
        )

    def sample(g, carry):
        gx = g // size_y
        gy = lax.rem(g, size_y)
        rows = pl.ds(pl.multiple_of(gy * win_y, 8), win_y)
        field = jnp.concatenate([field_ref[gx, j, rows, :] for j in range(planes)], axis=0)
        x_hi = xs_ref[g, 0:win_x]
        x_lo = xs_ref[g, win_x:]
        stack = [x_hi, x_hi, x_lo, x_lo] + [jnp.zeros_like(x_hi)] * (LANES // win_x - 4)
        values = mm(field.astype(bf16), jnp.concatenate(stack, axis=0))
        wave = wave_ref[g]
        mixed = values[0:win_y] * wave[0:1]
        for j in range(1, planes):
            mixed = mixed + values[j * win_y : (j + 1) * win_y] * wave[j : j + 1]
        line = jnp.sum(mixed * ys_ref[g], axis=0, keepdims=True)
        for i in range(size_z):
            part_ref[g * size_z + i] = line[:, i * atom_count : (i + 1) * atom_count]
        return carry

    lax.fori_loop(0, size_x * size_y, sample, 0)

    def send(o, carry):
        part_copy(o, lax.rem(me + o, devices)).start()
        return carry

    lax.fori_loop(1, devices, send, 0)

    lax.fori_loop(first_steps, cell_count // STEP_CELLS, pair_step, 0)

    invariant = None
    for d in range(3):
        v_hi, v_lo = two_pieces(vec_ref[d])
        vector = (mm(v_hi, wv_ref[...]) + mm(v_lo, wv_ref[...])) * (1.0 / math.sqrt(NBR))
        part = vector * vector
        invariant = part if invariant is None else invariant + part
    update = (msg_ref[...] + invariant).astype(bf16)
    out_ref[...] = (hidden_ref[...].astype(f32) + mm(update, wo_ref[...])).astype(bf16)

    def take(o, total):
        part_copy(o, lax.rem(me + o, devices)).wait()
        return total + held_ref[o]

    total = lax.fori_loop(1, devices, take, part_ref[me])
    rows = LANES // slots
    spot = iota((rows, LANES), 0) * slots + lax.rem(iota((rows, LANES), 1), slots)
    for chunk in range(atom_count // LANES):
        line = jnp.broadcast_to(total[:, chunk * LANES : (chunk + 1) * LANES], (rows, LANES))
        site_ref[chunk * rows : (chunk + 1) * rows, :] = lane_pick(line, spot)[:, :slots]


def shards(
    features,
    positions,
    grid_anchor,
    species,
    neighbours,
    neighbour_count,
    w_self,
    w_neighbour,
    w_radial,
    radial_rates,
    w_pair1,
    w_pair2,
    w_vector,
    w_out,
    w_charge,
    species_charge,
):
    cells_x, cells_y, cells_z, slot_count, channels = features.shape
    cells = (cells_x, cells_y, cells_z)
    cell_count = cells_x * cells_y * cells_z
    atom_count = cell_count * slot_count
    sizes = tuple(lax.axis_size(a) for a in AXES)
    devices = sizes[0] * sizes[1] * sizes[2]
    lengths = tuple(c * s * CELL for c, s in zip(cells, sizes))
    length_x, length_y, length_z = lengths
    screen = 2 * cells_y * CELL
    pairs = slot_count * NBR

    share = length_z // 2 // devices
    planes = 2 * share
    win_x = -(-(cells_x * CELL + 4) // 8) * 8
    win_y = -(-(cells_y * CELL + 4) // 8) * 8
    assert 2 * cells_z * slot_count == LANES and cells_y % 2 == 0
    assert LANES % (4 * win_x) == 0 and cells_z * CELL + 4 <= LANES
    all_modes = np.arange(length_z // 2)
    table_k = np.stack([all_modes, all_modes], axis=1)
    phase_c = np.stack([np.ones_like(all_modes), np.zeros_like(all_modes)], axis=1)
    table_k[0, 1] = length_z // 2
    phase_c[0, 1] = 1
    table_k = table_k.reshape(devices, planes)
    phase_c = phase_c.reshape(devices, planes).astype(np.float64)
    basis_x, modes_x = trig_basis(length_x)
    basis_y, modes_y = trig_basis(length_y)
    qx, sx = axis_terms(modes_x, length_x)
    qy, sy = axis_terms(modes_y, length_y)
    qz, sz = axis_terms(table_k, length_z)
    krow = np.stack([qy, sy], axis=1).astype(np.float32)
    zrow = np.stack([table_k, phase_c, 1.0 - phase_c, qz, sz], axis=2)
    plane_rows = -(-planes // 8) * 8
    zrow = np.concatenate([zrow, np.ones((devices, plane_rows - planes, 5))], axis=1)
    zrow = zrow.astype(np.float32)
    kx = np.stack([qx, sx]).astype(np.float32)
    grid_x, grid_y = cells_x * CELL, cells_y * CELL
    at_y = np.concatenate([(np.arange(win_y) + g * grid_y - 1) % length_y for g in range(sizes[1])])
    by = basis_y[:, at_y]
    per_block = LANES // (2 * win_x)
    blocks = -(-sizes[0] // per_block)
    forward = np.zeros((blocks, LANES, length_x))
    backward = np.zeros((length_x, sizes[0] * LANES))
    for g in range(sizes[0]):
        cols = basis_x[:, (np.arange(win_x) + g * grid_x - 1) % length_x]
        at = g % per_block * 2 * win_x
        forward[g // per_block, at : at + 2 * win_x] = np.concatenate([cols, cols], axis=1).T
        backward[:, g * LANES : g * LANES + 4 * win_x] = np.concatenate([cols] * 4, axis=1)
    tables = [jnp.asarray(zrow), jnp.asarray(krow), jnp.asarray(kx)]
    for table in (by, by.T, forward, backward):
        tables += host_pieces(table)

    vmem = pl.BlockSpec(memory_space=pltpu.VMEM)
    smem = pl.BlockSpec(memory_space=pltpu.SMEM)
    dma = pltpu.SemaphoreType.DMA
    groups = sizes[0] * sizes[1]
    lanes = sizes[2] * atom_count
    columns = (cells_x + 2) * (cells_y + 2)
    updated, site_potential = pl.pallas_call(
        functools.partial(layer_kernel, sizes, cells, lengths, screen, planes, win_x, win_y),
        out_shape=(
            jax.ShapeDtypeStruct((atom_count, channels), bf16),
            jax.ShapeDtypeStruct((cell_count, slot_count), f32),
        ),
        in_specs=[vmem] * 9 + [smem] + [vmem] * 5 + [smem] + [vmem] * 11,
        out_specs=(vmem, vmem),
        scratch_shapes=[
            pltpu.VMEM((4, atom_count), f32),
            pltpu.VMEM((devices, 4, atom_count), f32),
            pltpu.VMEM(tuple(c + 2 for c in cells) + (slot_count, channels), bf16),
            pltpu.VMEM((columns, (cells_z + 2) * slot_count, channels), f32),
            pltpu.VMEM((2, atom_count, channels), f32),
            pltpu.VMEM((cell_count, pairs), f32),
            pltpu.VMEM((cell_count, pairs), i32),
            pltpu.VMEM((cell_count, pairs), i32),
            pltpu.VMEM((cell_count, pairs), f32),
            pltpu.VMEM((planes * length_y, length_x), f32),
            pltpu.VMEM((columns // 2, 8, LANES), f32),
            pltpu.VMEM((cells_x * cells_y, 8, LANES), f32),
            pltpu.VMEM((cell_count, 8, pairs), f32),
            pltpu.VMEM((cell_count, 8, pairs), f32),
            pltpu.VMEM((sizes[2], plane_rows, LANES), f32),
            pltpu.VMEM((blocks, planes, sizes[1] * win_y, LANES), f32),
            pltpu.VMEM((planes * length_y, LANES), f32),
            pltpu.VMEM((sizes[0], planes, sizes[1] * win_y, LANES), f32),
            pltpu.VMEM((groups, plane_rows, lanes), f32),
            pltpu.VMEM((groups, 2 * win_x, lanes), bf16),
            pltpu.VMEM((groups, win_y, lanes), f32),
            pltpu.VMEM((devices, 1, atom_count), f32),
            pltpu.VMEM((devices, 1, atom_count), f32),
            pltpu.VMEM((atom_count, channels), f32),
            pltpu.VMEM((3, atom_count, channels), f32),
            pltpu.VMEM((2 * channels, 2 * channels), bf16),
            pltpu.VMEM((2 * channels, 2 * channels), bf16),
            dma((devices,)),
            dma((devices,)),
            dma((27,)),
            dma((27,)),
            dma((devices,)),
            dma((devices,)),
        ],
        name="fused_layer",
        compiler_params=pltpu.CompilerParams(
            has_side_effects=True, collective_id=0, vmem_limit_bytes=VMEM_BYTES
        ),
    )(
        features,
        features.reshape(atom_count, channels),
        positions.reshape(cell_count, 3 * slot_count),
        species.reshape(cell_count, slot_count),
        neighbours.reshape(cell_count, pairs),
        neighbour_count.reshape(cell_count, slot_count),
        w_self,
        w_neighbour,
        w_radial,
        radial_rates,
        w_pair1,
        w_pair2,
        w_vector,
        w_out,
        w_charge,
        species_charge,
        *tables,
    )
    return (
        updated.reshape(features.shape),
        site_potential.reshape(cells_x, cells_y, cells_z, slot_count),
    )


def solution(mesh):
    cells = P("gx", "gy", "gz", None)
    return jax.shard_map(
        shards,
        mesh=mesh,
        in_specs=(P("gx", "gy", "gz", None, None),) + (cells,) * 5 + (P(),) * 10,
        out_specs=(P("gx", "gy", "gz", None, None), cells),
        check_vma=False,
    )
```

```python
import functools
import math

import jax
import jax.numpy as jnp
import numpy as np
from jax import lax
from jax.experimental import pallas as pl
from jax.experimental.pallas import tpu as pltpu
from jax.sharding import PartitionSpec as P

NBR = 64
CELL = 8
LANES = 128
STEP_CELLS = 12
FIRST_LOADS = (2, 3, 1, 14, 15, 0)
VMEM_BYTES = 60 * 1024 * 1024
AXES = ("gx", "gy", "gz")

coulomb_scale = 0.25
smearing = 1.0
f32, bf16, i32 = jnp.float32, jnp.bfloat16, jnp.int32


def index_of(coords, sizes):
    return (coords[0] * sizes[1] + coords[1]) * sizes[2] + coords[2]


def iota(shape, axis):
    return lax.broadcasted_iota(i32, shape, axis)


def split_by(value, size):
    if size & (size - 1) == 0:
        shift = size.bit_length() - 1
        return lax.shift_right_logical(value, shift), value & (size - 1)
    high = jnp.floor((value.astype(f32) + 0.5) * (1.0 / size)).astype(i32)
    return high, value - high * size


def two_pieces(x):
    hi = x.astype(bf16)
    return hi, (x - hi.astype(f32)).astype(bf16)


def mm(a, b):
    return jnp.dot(a, b, preferred_element_type=f32)


def mm_nt(a, b):
    return lax.dot_general(a, b, (((1,), (1,)), ((), ())), preferred_element_type=f32)


def lane_pick(table, index):
    return jnp.take_along_axis(table, index, axis=1)


def silu_of_half(half):
    return (half + half * jnp.tanh(half)).astype(bf16)


def trig_basis(length):
    r = np.arange(length)
    rows = [np.cos(2 * np.pi * ((k * r) % length) / length) for k in range(length // 2 + 1)]
    rows += [np.sin(2 * np.pi * ((k * r) % length) / length) for k in range(1, length // 2)]
    modes = np.array(list(range(length // 2 + 1)) + list(range(1, length // 2)))
    return np.stack(rows), modes


def axis_terms(modes, length):
    wave = modes * (2.0 * np.pi / length)
    turn = np.exp(2j * np.pi * modes / length)
    modulus = np.abs(1 / 6 + 4 / 6 * turn + 1 / 6 * turn * turn) ** 2
    weight = np.where((modes == 0) | (2 * modes == length), 1.0, 2.0) / length
    return wave * wave, weight / modulus


def host_pieces(table):
    table = np.ascontiguousarray(table).astype(np.float32)
    hi = table.astype(jnp.bfloat16)
    lo = (table - hi.astype(np.float32)).astype(jnp.bfloat16)
    return hi, lo


def layer_kernel(
    sizes,
    cells,
    lengths,
    screen,
    planes,
    win_x,
    win_y,
    sources,
    out_ref,
    site_ref,
    atoms_ref,
    all_ref,
    near_ref,
    sent_ref,
    own_ref,
    which_ref,
    zlane_ref,
    column_ref,
    live_ref,
    green_ref,
    line_ref,
    mine_ref,
    basis_ref,
    reach_ref,
    ztab_ref,
    plane_ref,
    along_ref,
    field_ref,
    wave_ref,
    taps_ref,
    scaled_ref,
    xs_ref,
    ys_ref,
    part_ref,
    held_ref,
    msg_ref,
    vec_ref,
    bd1_ref,
    bd2_ref,
    asend,
    arecv,
    hsend,
    hrecv,
    psend,
    precv,
    entered,
    stage_sem,
    *staged,
):
    (
        feat_ref,
        hidden_ref,
        pos_ref,
        kind_ref,
        nbr_ref,
        count_ref,
        ws_ref,
        wn_ref,
        wr_ref,
        rates_ref,
        w1_ref,
        w2_ref,
        wv_ref,
        wo_ref,
        wc_ref,
        kinds_ref,
        zrow_ref,
        krow_ref,
        kx_ref,
        by_ref,
        byt_ref,
        bxt_h_ref,
        bxt_l_ref,
        bxq_h_ref,
        bxq_l_ref,
    ) = staged
    loads = [
        pltpu.make_async_copy(source, target, stage_sem.at[k])
        for k, (source, target) in enumerate(zip(sources, staged))
    ]
    for k in FIRST_LOADS:
        loads[k].start()
    size_x, size_y, size_z = sizes
    cells_x, cells_y, cells_z = cells
    length_x, length_y, length_z = lengths
    devices = size_x * size_y * size_z
    slots = feat_ref.shape[3]
    channels = feat_ref.shape[4]
    cell_count = cells_x * cells_y * cells_z
    atom_count = cell_count * slots
    pairs = slots * NBR
    half_pairs = pairs // 2
    run = cells_z * slots
    wide_y = cells_y + 2
    here = tuple(lax.axis_index(a) for a in AXES)
    me = index_of(here, sizes)

    offsets = [
        (a, b, c)
        for a in range(size_x)
        for b in range(size_y)
        for c in range(size_z)
        if (a, b, c) != (0, 0, 0)
    ]
    close = [
        all(step in (0, 1, size - 1) for step, size in zip(offset, sizes)) for offset in offsets
    ]
    offsets = [o for o, c in zip(offsets, close) if c] + [o for o, c in zip(offsets, close) if not c]
    close_count = sum(close)

    def moved(offset, sign):
        return tuple(
            lax.rem(at + (step if sign > 0 else size - step), size) if step else at
            for at, step, size in zip(here, offset, sizes)
        )

    def greet(semaphore):
        for offset in offsets[:close_count]:
            pl.semaphore_signal(
                semaphore, inc=1, device_id=moved(offset, 1), device_id_type=pl.DeviceIdType.MESH
            )

    barrier = pltpu.get_barrier_semaphore()
    greet(barrier)
    for k in range(len(loads)):
        if k not in FIRST_LOADS:
            loads[k].start()
    for k in FIRST_LOADS:
        loads[k].wait()

    pad_rows = jnp.zeros((LANES - cell_count, 1), f32)
    kinds = kind_ref[...].astype(f32)
    turned = [
        jnp.concatenate(
            [block, jnp.zeros((LANES - cell_count, block.shape[1]), f32)], axis=0
        ).T
        for block in (pos_ref[...], kinds)
    ]
    lane8 = iota((slots, LANES), 1)
    diagonal = (lane8 % slots) == iota((slots, LANES), 0)
    per_chunk = LANES // slots
    wc_rows = jnp.broadcast_to(wc_ref[...].reshape(1, channels), (slots, channels))
    readout = mm_nt(wc_rows, hidden_ref[...])

    def lined(block, chunk):
        picked = lane_pick(block, lane8 // slots + chunk * per_chunk)
        return jnp.sum(jnp.where(diagonal, picked, 0.0), axis=0, keepdims=True)

    for chunk in range(atom_count // LANES):
        where_to = slice(chunk * LANES, (chunk + 1) * LANES)
        for d in range(3):
            atoms_ref[d : d + 1, where_to] = lined(turned[0][d * slots : (d + 1) * slots], chunk)
        kind = lined(turned[1], chunk)
        charge = readout[0:1, where_to]
        for k in range(kinds_ref.shape[0]):
            charge = charge + jnp.where(kind == float(k), kinds_ref[k], 0.0)
        atoms_ref[3:4, where_to] = charge

    def atom_copy(at, peer, slot):
        return pltpu.make_async_remote_copy(
            src_ref=atoms_ref,
            dst_ref=all_ref.at[slot],
            send_sem=asend.at[at],
            recv_sem=arecv.at[at],
            device_id=peer,
            device_id_type=pl.DeviceIdType.MESH,
        )

    copies = []
    for shift in range(27):
        step = (shift // 9 - 1, shift // 3 % 3 - 1, shift % 3 - 1)
        if step == (0, 0, 0):
            continue
        source, target, peer = [], [], []
        for axis in range(3):
            size = cells[axis]
            if step[axis] == 0:
                source.append(pl.ds(0, size))
                target.append(pl.ds(1, size))
                peer.append(here[axis])
            elif step[axis] > 0:
                source.append(pl.ds(size - 1, 1))
                target.append(pl.ds(0, 1))
                peer.append(lax.rem(here[axis] + 1, sizes[axis]))
            else:
                source.append(pl.ds(0, 1))
                target.append(pl.ds(size + 1, 1))
                peer.append(lax.rem(here[axis] + sizes[axis] - 1, sizes[axis]))
        copies.append(
            pltpu.make_async_remote_copy(
                src_ref=feat_ref.at[tuple(source)],
                dst_ref=near_ref.at[tuple(target)],
                send_sem=hsend.at[shift],
                recv_sem=hrecv.at[shift],
                device_id=tuple(peer),
                device_id_type=pl.DeviceIdType.MESH,
            )
        )
    pl.semaphore_wait(barrier, close_count)
    for offset in offsets[:close_count]:
        atom_copy(index_of(offset, sizes), moved(offset, 1), me).start()
    rounds = max(size // 2 for size in sizes) - 1
    if rounds > 0:
        greet(entered.at[0])
    for copy in copies:
        copy.start()
    all_ref[me] = atoms_ref[...]

    for k in range(len(loads)):
        if k not in FIRST_LOADS:
            loads[k].wait()

    own = mm(hidden_ref[...], ws_ref[...]) * 0.5
    own_hi = own.astype(bf16).astype(f32)
    own_ref[0] = own_hi
    own_ref[1] = (own - own_hi).astype(bf16).astype(f32)

    no_block = jnp.zeros((channels, channels), bf16)
    for ref, target in ((w1_ref, bd1_ref), (w2_ref, bd2_ref)):
        weight = ref[...] * jnp.asarray(0.5, bf16)
        target[0:channels, 0:channels] = weight
        target[0:channels, channels:] = no_block
        target[channels:, 0:channels] = no_block
        target[channels:, channels:] = weight

    listed = nbr_ref[...]
    cell_id, slot_id = split_by(listed, slots)
    xy_id, z_id = split_by(cell_id, cells_z * size_z)
    x_id, y_id = split_by(xy_id, cells_y * size_y)
    row_xy, row_z = split_by(iota((cell_count, 1), 0), cells_z)
    row_x, row_y = split_by(row_xy, cells_y)
    steps = []
    for ids, local, axis in ((x_id, row_x, 0), (y_id, row_y, 1), (z_id, row_z, 2)):
        total = cells[axis] * sizes[axis]
        gap = ids - (local + here[axis] * cells[axis])
        gap = jnp.where(gap > 1, gap - total, gap)
        steps.append(jnp.where(gap < -1, gap + total, gap))
    which = ((steps[0] + 1) * 3 + steps[1] + 1) * (3 * slots) + (steps[2] + 1) * slots + slot_id
    octets = which_ref.shape
    which_ref[...] = which.astype(f32).reshape(octets)
    zlane = ((row_z + steps[2]) * slots + slot_id) & (LANES - 1)
    zlane_ref[...] = zlane.reshape(octets)
    column = (steps[0] + 1) * wide_y + row_y + 1 + steps[1]
    column_ref[...] = column.reshape(octets)
    lane_pair = iota((slots, pairs), 1)
    sel = jnp.where(lane_pair // NBR == iota((slots, pairs), 0), 1.0, 0.0)
    limit = mm(count_ref[...].astype(f32).astype(bf16), sel.astype(bf16))
    order = (iota((1, pairs), 1) % NBR).astype(f32)
    live_ref[...] = jnp.where(order < limit, 1.0, 0.0).reshape(octets)

    zrow = zrow_ref[me]
    kcol = krow_ref[...]
    for j in range(planes):
        q = kcol[:, 0:1] + zrow[j : j + 1, 3:4] + kx_ref[0:1, :]
        scale = kcol[:, 1:2] * zrow[j : j + 1, 4:5] * kx_ref[1:2, :]
        green = (coulomb_scale * 4.0 * math.pi) * jnp.exp(-0.5 * smearing * smearing * q)
        green = green * scale / (q + 1.0 / (screen * screen))
        green_ref[j * length_y : (j + 1) * length_y] = jnp.where(q == 0.0, 0.0, green)
    plane_ref[...] = jnp.zeros(plane_ref.shape, f32)
    for z in range(size_z):
        lane = (iota((1, LANES), 1) + (z * cells_z * CELL - 1)).astype(f32)
        turns = zrow[:, 0:1] * lane
        turns = turns - length_z * jnp.floor(turns * (1.0 / length_z))
        angle = (turns - 0.5 * length_z) * (2.0 * math.pi / length_z)
        ztab_ref[z] = -jnp.cos(angle) * zrow[:, 1:2] - jnp.sin(angle) * zrow[:, 2:3]

    for r in range(rounds):
        pl.semaphore_wait(entered.at[r], close_count)
        if r + 1 < rounds:
            greet(entered.at[r + 1])
    for offset in offsets[close_count:]:
        atom_copy(index_of(offset, sizes), moved(offset, 1), me).start()
    for offset in offsets[:close_count]:
        origin = moved(offset, -1)
        atom_copy(index_of(offset, sizes), origin, index_of(origin, sizes)).wait()

    lane4 = iota((4, LANES), 1)
    for x in range(cells_x + 2):
        for pair_y in range(wide_y // 2):
            halves = []
            for y in (2 * pair_y, 2 * pair_y + 1):
                spots, locals_ = [], []
                for at, axis in ((x, 0), (y, 1)):
                    size = cells[axis]
                    if at == 0:
                        spots.append(lax.rem(here[axis] + sizes[axis] - 1, sizes[axis]))
                        locals_.append(size - 1)
                    elif at == size + 1:
                        spots.append(lax.rem(here[axis] + 1, sizes[axis]))
                        locals_.append(0)
                    else:
                        spots.append(here[axis])
                        locals_.append(at - 1)
                column = locals_[0] * cells_y + locals_[1]
                start_lane = column * run
                block = pl.ds(start_lane // LANES * LANES, LANES)
                odd = start_lane % LANES != 0
                pieces = []
                for step_z in (0, 1, size_z - 1):
                    origin = index_of(
                        (spots[0], spots[1], lax.rem(here[2] + step_z, size_z)), sizes
                    )
                    piece = all_ref[origin, :, block]
                    if (step_z == 0) == odd:
                        piece = pltpu.roll(piece, run, 1)
                    pieces.append(piece)
                line = jnp.where(
                    lane4 < run, pieces[0], jnp.where(lane4 < run + slots, pieces[1], pieces[2])
                )
                halves.append(line)
                if 1 <= x <= cells_x and 1 <= y <= cells_y:
                    mine_ref[column] = jnp.concatenate([line, line], axis=0)
            line_ref[x * (wide_y // 2) + pair_y] = jnp.concatenate(halves, axis=0)

    sub8 = iota((slots, LANES), 0)
    row_d = iota((slots, 1), 0)
    box = jnp.where(
        row_d == 0,
        float(length_x),
        jnp.where(row_d == 1, float(length_y), float(length_z)),
    )
    box_inv = 1.0 / box
    rates = jnp.zeros((rates_ref.shape[0], 1), f32)
    for k in range(rates_ref.shape[0]):
        rates = jnp.where(iota(rates.shape, 0) == k, rates_ref[k], rates)
    sub_y = sub8 // 4

    def geometry(octet, carry):
        for r in range(8):
            place_cell(octet * 8 + r, octet, r)
        return carry

    def place_cell(c, octet, r):
        cz = lax.rem(c, cells_z)
        cxy = c // cells_z
        cx = cxy // cells_y
        for chunk in range(pairs // LANES):
            part = pl.ds(chunk * LANES, LANES)
            spot = jnp.broadcast_to(zlane_ref[octet, r : r + 1, part], (slots, LANES))
            column = jnp.broadcast_to(column_ref[octet, r : r + 1, part], (slots, LANES)) - sub_y
            live = live_ref[octet, r : r + 1, part]
            which = which_ref[octet, r : r + 1, part]
            found = jnp.zeros((slots, LANES), f32)
            for dx in range(3):
                for pair_y in range(wide_y // 2):
                    table = line_ref[(cx + dx) * (wide_y // 2) + pair_y]
                    picked = lane_pick(table, spot)
                    found = jnp.where(column == dx * wide_y + 2 * pair_y, picked, found)
            found = found + pltpu.roll(found, 4, 0)
            own_spot = cz * slots + (lane8 + chunk * LANES) // NBR
            displace = found - lane_pick(mine_ref[cxy], own_spot)
            displace = displace - box * jnp.floor(displace * box_inv + 0.5)
            scaled = jnp.where(row_d < 3, displace * (1.0 / CELL), 0.0)
            square = jnp.sum(scaled * scaled, axis=0, keepdims=True)
            basis_ref[c, :, part] = jnp.exp(-square * rates)
            reach = jnp.where(row_d == 3, 1.0, scaled) * live
            reach_ref[c, :, part] = jnp.where(row_d == 4, which, reach)

    lax.fori_loop(0, cell_count // 8, geometry, 0)

    for copy in copies:
        copy.wait()
    for x in range(cells_x + 2):
        for y in range(wide_y):
            if 1 <= x <= cells_x and 1 <= y <= cells_y:
                blocks = [
                    near_ref[x, y, 0:1],
                    feat_ref[x - 1, y - 1],
                    near_ref[x, y, cells_z + 1 :],
                ]
            else:
                blocks = [near_ref[x, y]]
            line = [b.astype(f32).reshape(b.shape[0] * slots, channels) for b in blocks]
            line = jnp.concatenate(line, axis=0).astype(bf16)
            sent_ref[x * wide_y + y] = mm(line, wn_ref[...]).astype(bf16).astype(f32) * 0.5

    hot_rows = 27 * slots
    even_rows = hot_rows // 16 * 16
    hot_ids = iota((even_rows, 1), 0).astype(f32).astype(bf16)
    last_ids = (iota((hot_rows - even_rows, 1), 0) + even_rows).astype(f32)
    wr_rows = wr_ref[...].astype(f32) * 0.5
    sel_tile = jnp.concatenate([sel, sel], axis=0).astype(bf16)
    sub_h = iota((slots, half_pairs), 0)
    slot_h = iota((slots, half_pairs), 1) // NBR
    in_low = slot_h == sub_h
    in_high = slot_h == sub_h - slots // 2

    def pair_step(step, carry):
        rows = []
        for u in range(STEP_CELLS):
            c = step * STEP_CELLS + u
            cz = lax.rem(c, cells_z)
            cxy = c // cells_z
            cy = lax.rem(cxy, cells_y)
            cx = cxy // cells_y
            at = pl.ds(pl.multiple_of(cz * slots, slots), 3 * slots)
            mine = pl.ds(pl.multiple_of(c * slots, slots), slots)
            parts = []
            for dx in range(3):
                for dy in range(3):
                    parts.append(sent_ref[(cx + dx) * wide_y + cy + dy, at, :])
            parts += [wr_rows, own_ref[0, mine, :], own_ref[1, mine, :]]
            table = jnp.concatenate(parts, axis=0).astype(bf16).T
            which = reach_ref[c, 4:5, :]
            hot = jnp.where(
                hot_ids == which.astype(bf16), jnp.asarray(1.0, bf16), jnp.asarray(0.0, bf16)
            )
            last = jnp.where(last_ids == which, 1.0, 0.0)
            tile = jnp.concatenate([last, basis_ref[c]], axis=0).astype(bf16)
            rhs = jnp.concatenate([hot, tile, sel_tile], axis=0)
            latent = silu_of_half(mm(table, rhs)).T
            rows.append(jnp.concatenate([latent[:half_pairs], latent[half_pairs:]], axis=1))
        second = silu_of_half(mm(jnp.concatenate(rows, axis=0), bd1_ref[...]))
        third = silu_of_half(mm(second, bd2_ref[...]))
        for u in range(STEP_CELLS):
            c = step * STEP_CELLS + u
            mine = pl.ds(pl.multiple_of(c * slots, slots), slots)
            weights = []
            for r in (3, 0, 1, 2):
                low = reach_ref[c, r : r + 1, 0:half_pairs]
                high = reach_ref[c, r : r + 1, half_pairs:]
                full = jnp.where(in_low, low, jnp.where(in_high, high, 0.0))
                if r == 3:
                    weights.append(full)
                else:
                    full_hi = full.astype(bf16).astype(f32)
                    weights += [full_hi, full - full_hi]
            weights = jnp.concatenate(weights, axis=0).astype(bf16)
            sums = mm(weights, third[u * half_pairs : (u + 1) * half_pairs])
            rest = []
            for r in range(7):
                block = sums[r * slots : (r + 1) * slots]
                rest.append(
                    jnp.where(row_d < slots // 2, block[:, :channels], block[:, channels:])
                )
            msg_ref[mine, :] = rest[0] * (1.0 / NBR)
            for d in range(3):
                vec_ref[d, mine, :] = rest[1 + 2 * d] + rest[2 + 2 * d]
        return carry

    lanes = size_z * atom_count

    def spread(turn, carry):
        gx = lax.rem(here[0] + size_x - turn // size_y, size_x)
        gy = lax.rem(here[1] + size_y - lax.rem(turn, size_y), size_y)
        g = gx * size_y + gy
        base = g * size_z
        step_x, step_y = turn // size_y, lax.rem(turn, size_y)
        far_group = jnp.logical_or(
            jnp.logical_and(step_x > 1, step_x < size_x - 1),
            jnp.logical_and(step_y > 1, step_y < size_y - 1),
        )
        for z in range(size_z):
            gz = lax.rem(here[2] + size_z - z, size_z)
            copy = atom_copy(turn * size_z + z, (gx, gy, gz), base + gz)
            if z in (0, 1, size_z - 1):
                pl.when(far_group)(copy.wait)
            else:
                copy.wait()
        atoms = jnp.concatenate([all_ref[base + i] for i in range(size_z)], axis=1)
        whole = jnp.floor(atoms)
        f = atoms - whole
        sq = f * f
        cube = sq * f
        rem = 1.0 - f
        taps = [
            rem * rem * rem * (1.0 / 6.0),
            (3.0 * cube - 6.0 * sq + 4.0) * (1.0 / 6.0),
            (-3.0 * cube + 3.0 * sq + 3.0 * f + 1.0) * (1.0 / 6.0),
            cube * (1.0 / 6.0),
        ]
        for t in range(4):
            taps_ref[t] = taps[t]
        taps_ref[4] = whole
        first_x = (gx * (cells_x * CELL)).astype(f32)
        first_y = (gy * (cells_y * CELL)).astype(f32)
        off_x = iota((win_x, 1), 0).astype(f32).astype(bf16) - (taps_ref[4, 0:1, :] - first_x).astype(bf16)
        x_hi = jnp.zeros((win_x, lanes), bf16)
        x_lo = jnp.zeros((win_x, lanes), bf16)
        for t in range(4):
            hit = off_x == jnp.asarray(t, bf16)
            t_hi, t_lo = two_pieces(taps_ref[t, 0:1, :])
            x_hi = jnp.where(hit, jnp.broadcast_to(t_hi, hit.shape), x_hi)
            x_lo = jnp.where(hit, jnp.broadcast_to(t_lo, hit.shape), x_lo)
        off_y = iota((win_y, 1), 0).astype(f32) - (taps_ref[4, 1:2, :] - first_y)
        rows_y = jnp.zeros((win_y, lanes), f32)
        for t in range(4):
            rows_y = jnp.where(off_y == float(t), taps_ref[t, 1:2, :], rows_y)
        waves = []
        for z in range(size_z):
            table = ztab_ref[z]
            for chunk in range(atom_count // LANES):
                part = slice(z * atom_count + chunk * LANES, z * atom_count + (chunk + 1) * LANES)
                spot = (taps_ref[4, 2:3, part] - float(z * cells_z * CELL)).astype(i32)
                spot = jnp.broadcast_to(spot, table.shape)
                wave = None
                for t in range(4):
                    term = lane_pick(table, spot + t) * taps_ref[t, 2:3, part]
                    wave = term if wave is None else wave + term
                waves.append(wave)
        wave = jnp.concatenate(waves, axis=1)
        wave_ref[g] = wave
        ys_ref[g] = rows_y
        rows_x = jnp.concatenate([x_hi, x_lo], axis=0)
        xs_ref[g] = rows_x
        scaled_ref[...] = wave * atoms[3:4]
        left = jnp.concatenate([rows_y * scaled_ref[j : j + 1, :] for j in range(planes)], axis=0)
        l_hi, l_lo = two_pieces(left)
        res = mm_nt(l_hi, rows_x) + mm_nt(l_lo, rows_x)
        per_block = LANES // (2 * win_x)
        res = jnp.concatenate([res, jnp.zeros((res.shape[0], LANES - 2 * win_x), f32)], axis=1)
        res = pltpu.roll(res, lax.rem(gx, per_block) * (2 * win_x), 1)
        rows = pl.ds(pl.multiple_of(gy * win_y, 8), win_y)
        for j in range(planes):
            plane_ref[gx // per_block, j, rows, :] += res[j * win_y : (j + 1) * win_y]
        return carry

    lax.fori_loop(0, size_x * size_y, spread, 0)

    spectrum = None
    for block in range(plane_ref.shape[0]):
        for j in range(0, planes, 2):
            p_hi, p_lo = two_pieces(
                jnp.concatenate([plane_ref[block, j], plane_ref[block, j + 1]], axis=1)
            )
            both = mm(by_ref[0], p_hi) + mm(by_ref[0], p_lo) + mm(by_ref[1], p_hi)
            along_ref[j * length_y : (j + 1) * length_y, :] = both[:, :LANES]
            along_ref[(j + 1) * length_y : (j + 2) * length_y, :] = both[:, LANES:]
        a_hi, a_lo = two_pieces(along_ref[...])
        bxt_h = bxt_h_ref[block]
        part = mm(jnp.concatenate([a_hi, a_lo], axis=1), jnp.concatenate([bxt_h, bxt_h], axis=0))
        part = part + mm(a_hi, bxt_l_ref[block])
        spectrum = part if spectrum is None else spectrum + part
    s_hi, s_lo = two_pieces(spectrum * green_ref[...])
    lane_x = iota((1, 2 * LANES), 1) % (2 * win_x) < win_x
    for gx in range(0, size_x, 2):
        cols = slice(gx * LANES, (gx + 2) * LANES)
        back = (
            mm(s_hi, bxq_h_ref[:, cols]) + mm(s_lo, bxq_h_ref[:, cols]) + mm(s_hi, bxq_l_ref[:, cols])
        )
        b_hi, b_lo = two_pieces(back)
        for j in range(planes):
            rows = slice(j * length_y, (j + 1) * length_y)
            value = mm(
                byt_ref[...], jnp.concatenate([b_hi[rows], b_lo[rows], b_hi[rows]], axis=0)
            )
            v_hi = value.astype(bf16).astype(f32)
            value = jnp.where(lane_x, v_hi, value - v_hi)
            field_ref[gx, j] = value[:, :LANES]
            field_ref[gx + 1, j] = value[:, LANES:]

    def part_copy(o, peer):
        return pltpu.make_async_remote_copy(
            src_ref=part_ref.at[index_of(peer, sizes)],
            dst_ref=held_ref.at[o],
            send_sem=psend.at[o],
            recv_sem=precv.at[o],
            device_id=peer,
            device_id_type=pl.DeviceIdType.MESH,
        )

    def sample(g, carry):
        gx = g // size_y
        gy = lax.rem(g, size_y)
        rows = pl.ds(pl.multiple_of(gy * win_y, 8), win_y)
        field = jnp.concatenate([field_ref[gx, j, rows, :] for j in range(planes)], axis=0)
        x_hi = xs_ref[g, 0:win_x]
        x_lo = xs_ref[g, win_x:]
        stack = [x_hi, x_hi, x_lo, x_lo] + [jnp.zeros_like(x_hi)] * (LANES // win_x - 4)
        values = mm(field.astype(bf16), jnp.concatenate(stack, axis=0))
        mixed = values[0:win_y] * wave_ref[g, 0:1, :]
        for j in range(1, planes):
            mixed = mixed + values[j * win_y : (j + 1) * win_y] * wave_ref[g, j : j + 1, :]
        line = jnp.sum(mixed * ys_ref[g], axis=0, keepdims=True)
        for i in range(size_z):
            part_ref[g * size_z + i] = line[:, i * atom_count : (i + 1) * atom_count]
        return carry

    lax.fori_loop(0, size_x * size_y, sample, 0, unroll=4)

    for offset in offsets:
        part_copy(index_of(offset, sizes), moved(offset, 1)).start()

    lax.fori_loop(0, cell_count // STEP_CELLS, pair_step, 0)

    wv_twice = jnp.concatenate([wv_ref[...], wv_ref[...]], axis=0)
    invariant = None
    for d in range(3):
        vector = mm(jnp.concatenate(two_pieces(vec_ref[d]), axis=1), wv_twice)
        vector = vector * (1.0 / math.sqrt(NBR))
        part = vector * vector
        invariant = part if invariant is None else invariant + part
    update = (msg_ref[...] + invariant).astype(bf16)
    out_ref[...] = (hidden_ref[...].astype(f32) + mm(update, wo_ref[...])).astype(bf16)

    for offset in offsets:
        part_copy(index_of(offset, sizes), moved(offset, 1)).wait()
    held_ref[0] = part_ref[me]
    total = jnp.sum(held_ref[...], axis=0)
    rows = LANES // slots
    spot = iota((rows, LANES), 0) * slots + lax.rem(iota((rows, LANES), 1), slots)
    for chunk in range(atom_count // LANES):
        line = jnp.broadcast_to(total[:, chunk * LANES : (chunk + 1) * LANES], (rows, LANES))
        site_ref[chunk * rows : (chunk + 1) * rows, :] = lane_pick(line, spot)[:, :slots]


def staged_kernel(*args):
    count = args[7]
    layer_kernel(*args[:7], args[8 : 8 + count], *args[8 + count :])


def shards(
    features,
    positions,
    grid_anchor,
    species,
    neighbours,
    neighbour_count,
    w_self,
    w_neighbour,
    w_radial,
    radial_rates,
    w_pair1,
    w_pair2,
    w_vector,
    w_out,
    w_charge,
    species_charge,
):
    cells_x, cells_y, cells_z, slot_count, channels = features.shape
    cells = (cells_x, cells_y, cells_z)
    cell_count = cells_x * cells_y * cells_z
    atom_count = cell_count * slot_count
    sizes = tuple(lax.axis_size(a) for a in AXES)
    devices = sizes[0] * sizes[1] * sizes[2]
    lengths = tuple(c * s * CELL for c, s in zip(cells, sizes))
    length_x, length_y, length_z = lengths
    screen = 2 * cells_y * CELL
    pairs = slot_count * NBR

    share = length_z // 2 // devices
    planes = 2 * share
    win_x = -(-(cells_x * CELL + 4) // 8) * 8
    win_y = -(-(cells_y * CELL + 4) // 8) * 8
    assert 2 * cells_z * slot_count == LANES and cells_y % 2 == 0
    assert LANES % (4 * win_x) == 0 and cells_z * CELL + 4 <= LANES
    all_modes = np.arange(length_z // 2)
    table_k = np.stack([all_modes, all_modes], axis=1)
    phase_c = np.stack([np.ones_like(all_modes), np.zeros_like(all_modes)], axis=1)
    table_k[0, 1] = length_z // 2
    phase_c[0, 1] = 1
    table_k = table_k.reshape(devices, planes)
    phase_c = phase_c.reshape(devices, planes).astype(np.float64)
    basis_x, modes_x = trig_basis(length_x)
    basis_y, modes_y = trig_basis(length_y)
    qx, sx = axis_terms(modes_x, length_x)
    qy, sy = axis_terms(modes_y, length_y)
    qz, sz = axis_terms(table_k, length_z)
    krow = np.stack([qy, sy], axis=1).astype(np.float32)
    zrow = np.stack([table_k, phase_c, 1.0 - phase_c, qz, sz], axis=2)
    plane_rows = -(-planes // 8) * 8
    zrow = np.concatenate([zrow, np.ones((devices, plane_rows - planes, 5))], axis=1)
    zrow = zrow.astype(np.float32)
    kx = np.stack([qx, sx]).astype(np.float32)
    grid_x, grid_y = cells_x * CELL, cells_y * CELL
    at_y = np.concatenate([(np.arange(win_y) + g * grid_y - 1) % length_y for g in range(sizes[1])])
    by = basis_y[:, at_y]
    per_block = LANES // (2 * win_x)
    blocks = -(-sizes[0] // per_block)
    forward = np.zeros((blocks, LANES, length_x))
    backward = np.zeros((length_x, sizes[0] * LANES))
    for g in range(sizes[0]):
        cols = basis_x[:, (np.arange(win_x) + g * grid_x - 1) % length_x]
        at = g % per_block * 2 * win_x
        forward[g // per_block, at : at + 2 * win_x] = np.concatenate([cols, cols], axis=1).T
        backward[:, g * LANES : g * LANES + 4 * win_x] = np.concatenate([cols] * 4, axis=1)
    tables = [jnp.asarray(zrow), jnp.asarray(krow), jnp.asarray(kx)]
    by_hi, by_lo = host_pieces(by)
    tables.append(np.stack([by_hi, by_lo]))
    tables.append(np.concatenate([by_hi.T, by_hi.T, by_lo.T], axis=1))
    for table in (forward, backward):
        tables += host_pieces(table)
    tables = [jnp.asarray(t) for t in tables]

    operands = (
        features,
        features.reshape(atom_count, channels),
        positions.reshape(cell_count, 3 * slot_count),
        species.reshape(cell_count, slot_count),
        neighbours.reshape(cell_count, pairs),
        neighbour_count.reshape(cell_count, slot_count),
        w_self,
        w_neighbour,
        w_radial,
        radial_rates,
        w_pair1,
        w_pair2,
        w_vector,
        w_out,
        w_charge,
        species_charge,
        *tables,
    )
    vmem = pl.BlockSpec(memory_space=pltpu.VMEM)
    dma = pltpu.SemaphoreType.DMA
    groups = sizes[0] * sizes[1]
    lanes = sizes[2] * atom_count
    columns = (cells_x + 2) * (cells_y + 2)
    updated, site_potential = pl.pallas_call(
        functools.partial(
            staged_kernel, sizes, cells, lengths, screen, planes, win_x, win_y, len(operands)
        ),
        out_shape=(
            jax.ShapeDtypeStruct((atom_count, channels), bf16),
            jax.ShapeDtypeStruct((cell_count, slot_count), f32),
        ),
        in_specs=[pl.BlockSpec(memory_space=pl.ANY)] * len(operands),
        out_specs=(vmem, vmem),
        scratch_shapes=[
            pltpu.VMEM((4, atom_count), f32),
            pltpu.VMEM((devices, 4, atom_count), f32),
            pltpu.VMEM(tuple(c + 2 for c in cells) + (slot_count, channels), bf16),
            pltpu.VMEM((columns, (cells_z + 2) * slot_count, channels), f32),
            pltpu.VMEM((2, atom_count, channels), f32),
            pltpu.VMEM((cell_count // 8, 8, pairs), f32),
            pltpu.VMEM((cell_count // 8, 8, pairs), i32),
            pltpu.VMEM((cell_count // 8, 8, pairs), i32),
            pltpu.VMEM((cell_count // 8, 8, pairs), f32),
            pltpu.VMEM((planes * length_y, length_x), f32),
            pltpu.VMEM((columns // 2, 8, LANES), f32),
            pltpu.VMEM((cells_x * cells_y, 8, LANES), f32),
            pltpu.VMEM((cell_count, 8, pairs), f32),
            pltpu.VMEM((cell_count, 8, pairs), f32),
            pltpu.VMEM((sizes[2], plane_rows, LANES), f32),
            pltpu.VMEM((blocks, planes, sizes[1] * win_y, LANES), f32),
            pltpu.VMEM((planes * length_y, LANES), f32),
            pltpu.VMEM((sizes[0], planes, sizes[1] * win_y, LANES), f32),
            pltpu.VMEM((groups, plane_rows, lanes), f32),
            pltpu.VMEM((5, 4, lanes), f32),
            pltpu.VMEM((plane_rows, lanes), f32),
            pltpu.VMEM((groups, 2 * win_x, lanes), bf16),
            pltpu.VMEM((groups, win_y, lanes), f32),
            pltpu.VMEM((devices, 1, atom_count), f32),
            pltpu.VMEM((devices, 1, atom_count), f32),
            pltpu.VMEM((atom_count, channels), f32),
            pltpu.VMEM((3, atom_count, channels), f32),
            pltpu.VMEM((2 * channels, 2 * channels), bf16),
            pltpu.VMEM((2 * channels, 2 * channels), bf16),
            dma((devices,)),
            dma((devices,)),
            dma((27,)),
            dma((27,)),
            dma((devices,)),
            dma((devices,)),
            pltpu.SemaphoreType.REGULAR((max(max(size // 2 for size in sizes) - 1, 1),)),
            dma((len(operands),)),
        ]
        + [
            (pltpu.SMEM if a is radial_rates or a is species_charge else pltpu.VMEM)(
                a.shape, a.dtype
            )
            for a in operands
        ],
        name="fused_layer",
        compiler_params=pltpu.CompilerParams(
            has_side_effects=True, collective_id=0, vmem_limit_bytes=VMEM_BYTES
        ),
    )(*operands)
    return (
        updated.reshape(features.shape),
        site_potential.reshape(cells_x, cells_y, cells_z, slot_count),
    )


def solution(mesh):
    cells = P("gx", "gy", "gz", None)
    return jax.shard_map(
        shards,
        mesh=mesh,
        in_specs=(P("gx", "gy", "gz", None, None),) + (cells,) * 5 + (P(),) * 10,
        out_specs=(P("gx", "gy", "gz", None, None), cells),
        check_vma=False,
    )
```

```python
import functools
import math

import jax
import jax.numpy as jnp
import numpy as np
from jax import lax
from jax.experimental import pallas as pl
from jax.experimental.pallas import tpu as pltpu
from jax.sharding import PartitionSpec as P

NBR = 64
CELL = 8
LANES = 128
STEP_CELLS = 12
FIRST_LOADS = (2, 3, 1, 14, 15, 0)
VMEM_BYTES = 60 * 1024 * 1024
AXES = ("gx", "gy", "gz")

coulomb_scale = 0.25
smearing = 1.0
f32, bf16, i32 = jnp.float32, jnp.bfloat16, jnp.int32


def index_of(coords, sizes):
    return (coords[0] * sizes[1] + coords[1]) * sizes[2] + coords[2]


def iota(shape, axis):
    return lax.broadcasted_iota(i32, shape, axis)


def split_by(value, size):
    if size & (size - 1) == 0:
        shift = size.bit_length() - 1
        return lax.shift_right_logical(value, shift), value & (size - 1)
    high = jnp.floor((value.astype(f32) + 0.5) * (1.0 / size)).astype(i32)
    return high, value - high * size


def two_pieces(x):
    hi = x.astype(bf16)
    return hi, (x - hi.astype(f32)).astype(bf16)


def mm(a, b):
    return jnp.dot(a, b, preferred_element_type=f32)


def mm_nt(a, b):
    return lax.dot_general(a, b, (((1,), (1,)), ((), ())), preferred_element_type=f32)


def lane_pick(table, index):
    dims = lax.GatherDimensionNumbers(
        offset_dims=(),
        collapsed_slice_dims=(1,),
        start_index_map=(1,),
        operand_batching_dims=(0,),
        start_indices_batching_dims=(0,),
    )
    return lax.gather(
        table, index[..., None], dims, (1, 1), mode=lax.GatherScatterMode.PROMISE_IN_BOUNDS
    )


def silu_of_half(half):
    return (half + half * jnp.tanh(half)).astype(bf16)


def trig_basis(length):
    r = np.arange(length)
    rows = [np.cos(2 * np.pi * ((k * r) % length) / length) for k in range(length // 2 + 1)]
    rows += [np.sin(2 * np.pi * ((k * r) % length) / length) for k in range(1, length // 2)]
    modes = np.array(list(range(length // 2 + 1)) + list(range(1, length // 2)))
    return np.stack(rows), modes


def axis_terms(modes, length):
    wave = modes * (2.0 * np.pi / length)
    turn = np.exp(2j * np.pi * modes / length)
    modulus = np.abs(1 / 6 + 4 / 6 * turn + 1 / 6 * turn * turn) ** 2
    weight = np.where((modes == 0) | (2 * modes == length), 1.0, 2.0) / length
    return wave * wave, weight / modulus


def host_pieces(table):
    table = np.ascontiguousarray(table).astype(np.float32)
    hi = table.astype(jnp.bfloat16)
    lo = (table - hi.astype(np.float32)).astype(jnp.bfloat16)
    return hi, lo


def layer_kernel(
    sizes,
    cells,
    lengths,
    screen,
    planes,
    win_x,
    win_y,
    sources,
    out_ref,
    site_ref,
    atoms_ref,
    all_ref,
    near_ref,
    sent_ref,
    own_ref,
    which_ref,
    zlane_ref,
    column_ref,
    live_ref,
    green_ref,
    line_ref,
    mine_ref,
    basis_ref,
    reach_ref,
    ztab_ref,
    plane_ref,
    along_ref,
    field_ref,
    wave_ref,
    taps_ref,
    scaled_ref,
    xs_ref,
    ys_ref,
    part_ref,
    held_ref,
    msg_ref,
    vec_ref,
    bd1_ref,
    bd2_ref,
    asend,
    arecv,
    hsend,
    hrecv,
    psend,
    precv,
    entered,
    stage_sem,
    *staged,
):
    (
        feat_ref,
        hidden_ref,
        pos_ref,
        kind_ref,
        nbr_ref,
        count_ref,
        ws_ref,
        wn_ref,
        wr_ref,
        rates_ref,
        w1_ref,
        w2_ref,
        wv_ref,
        wo_ref,
        wc_ref,
        kinds_ref,
        zrow_ref,
        krow_ref,
        kx_ref,
        by_ref,
        byt_ref,
        bxt_h_ref,
        bxt_l_ref,
        bxq_h_ref,
        bxq_l_ref,
    ) = staged
    loads = [
        pltpu.make_async_copy(source, target, stage_sem.at[k])
        for k, (source, target) in enumerate(zip(sources, staged))
    ]
    for k in FIRST_LOADS:
        loads[k].start()
    size_x, size_y, size_z = sizes
    cells_x, cells_y, cells_z = cells
    length_x, length_y, length_z = lengths
    devices = size_x * size_y * size_z
    slots = feat_ref.shape[3]
    channels = feat_ref.shape[4]
    cell_count = cells_x * cells_y * cells_z
    atom_count = cell_count * slots
    pairs = slots * NBR
    half_pairs = pairs // 2
    run = cells_z * slots
    wide_y = cells_y + 2
    here = tuple(lax.axis_index(a) for a in AXES)
    me = index_of(here, sizes)

    offsets = [
        (a, b, c)
        for a in range(size_x)
        for b in range(size_y)
        for c in range(size_z)
        if (a, b, c) != (0, 0, 0)
    ]
    close = [
        all(step in (0, 1, size - 1) for step, size in zip(offset, sizes)) for offset in offsets
    ]
    offsets = [o for o, c in zip(offsets, close) if c] + [o for o, c in zip(offsets, close) if not c]
    close_count = sum(close)

    def moved(offset, sign):
        return tuple(
            lax.rem(at + (step if sign > 0 else size - step), size) if step else at
            for at, step, size in zip(here, offset, sizes)
        )

    def greet(semaphore):
        for offset in offsets[:close_count]:
            pl.semaphore_signal(
                semaphore, inc=1, device_id=moved(offset, 1), device_id_type=pl.DeviceIdType.MESH
            )

    barrier = pltpu.get_barrier_semaphore()
    greet(barrier)
    for k in range(len(loads)):
        if k not in FIRST_LOADS:
            loads[k].start()
    for k in FIRST_LOADS:
        loads[k].wait()

    pad_rows = jnp.zeros((LANES - cell_count, 1), f32)
    kinds = kind_ref[...].astype(f32)
    turned = [
        jnp.concatenate(
            [block, jnp.zeros((LANES - cell_count, block.shape[1]), f32)], axis=0
        ).T
        for block in (pos_ref[...], kinds)
    ]
    lane8 = iota((slots, LANES), 1)
    diagonal = (lane8 % slots) == iota((slots, LANES), 0)
    per_chunk = LANES // slots
    wc_rows = jnp.broadcast_to(wc_ref[...].reshape(1, channels), (slots, channels))
    readout = mm_nt(wc_rows, hidden_ref[...])

    def lined(block, chunk):
        picked = lane_pick(block, lane8 // slots + chunk * per_chunk)
        return jnp.sum(jnp.where(diagonal, picked, 0.0), axis=0, keepdims=True)

    for chunk in range(atom_count // LANES):
        where_to = slice(chunk * LANES, (chunk + 1) * LANES)
        for d in range(3):
            atoms_ref[d : d + 1, where_to] = lined(turned[0][d * slots : (d + 1) * slots], chunk)
        kind = lined(turned[1], chunk)
        charge = readout[0:1, where_to]
        for k in range(kinds_ref.shape[0]):
            charge = charge + jnp.where(kind == float(k), kinds_ref[k], 0.0)
        atoms_ref[3:4, where_to] = charge

    def atom_copy(at, peer, slot):
        return pltpu.make_async_remote_copy(
            src_ref=atoms_ref,
            dst_ref=all_ref.at[slot],
            send_sem=asend.at[at],
            recv_sem=arecv.at[at],
            device_id=peer,
            device_id_type=pl.DeviceIdType.MESH,
        )

    copies = []
    for shift in range(27):
        step = (shift // 9 - 1, shift // 3 % 3 - 1, shift % 3 - 1)
        if step == (0, 0, 0):
            continue
        source, target, peer = [], [], []
        for axis in range(3):
            size = cells[axis]
            if step[axis] == 0:
                source.append(pl.ds(0, size))
                target.append(pl.ds(1, size))
                peer.append(here[axis])
            elif step[axis] > 0:
                source.append(pl.ds(size - 1, 1))
                target.append(pl.ds(0, 1))
                peer.append(lax.rem(here[axis] + 1, sizes[axis]))
            else:
                source.append(pl.ds(0, 1))
                target.append(pl.ds(size + 1, 1))
                peer.append(lax.rem(here[axis] + sizes[axis] - 1, sizes[axis]))
        copies.append(
            pltpu.make_async_remote_copy(
                src_ref=feat_ref.at[tuple(source)],
                dst_ref=near_ref.at[tuple(target)],
                send_sem=hsend.at[shift],
                recv_sem=hrecv.at[shift],
                device_id=tuple(peer),
                device_id_type=pl.DeviceIdType.MESH,
            )
        )
    pl.semaphore_wait(barrier, close_count)
    for offset in offsets[:close_count]:
        atom_copy(index_of(offset, sizes), moved(offset, 1), me).start()
    rounds = max(size // 2 for size in sizes) - 1
    if rounds > 0:
        greet(entered.at[0])
    for copy in copies:
        copy.start()
    all_ref[me] = atoms_ref[...]

    for k in range(len(loads)):
        if k not in FIRST_LOADS:
            loads[k].wait()

    own = mm(hidden_ref[...], ws_ref[...]) * 0.5
    own_hi = own.astype(bf16).astype(f32)
    own_ref[0] = own_hi
    own_ref[1] = (own - own_hi).astype(bf16).astype(f32)

    no_block = jnp.zeros((channels, channels), bf16)
    for ref, target in ((w1_ref, bd1_ref), (w2_ref, bd2_ref)):
        weight = ref[...] * jnp.asarray(0.5, bf16)
        target[0:channels, 0:channels] = weight
        target[0:channels, channels:] = no_block
        target[channels:, 0:channels] = no_block
        target[channels:, channels:] = weight

    listed = nbr_ref[...]
    cell_id, slot_id = split_by(listed, slots)
    xy_id, z_id = split_by(cell_id, cells_z * size_z)
    x_id, y_id = split_by(xy_id, cells_y * size_y)
    row_xy, row_z = split_by(iota((cell_count, 1), 0), cells_z)
    row_x, row_y = split_by(row_xy, cells_y)
    steps = []
    for ids, local, axis in ((x_id, row_x, 0), (y_id, row_y, 1), (z_id, row_z, 2)):
        total = cells[axis] * sizes[axis]
        gap = ids - (local + here[axis] * cells[axis])
        gap = jnp.where(gap > 1, gap - total, gap)
        steps.append(jnp.where(gap < -1, gap + total, gap))
    which = ((steps[0] + 1) * 3 + steps[1] + 1) * (3 * slots) + (steps[2] + 1) * slots + slot_id
    octets = which_ref.shape
    which_ref[...] = which.astype(f32).reshape(octets)
    zlane = ((row_z + steps[2]) * slots + slot_id) & (LANES - 1)
    zlane_ref[...] = zlane.reshape(octets)
    column = (steps[0] + 1) * wide_y + row_y + 1 + steps[1]
    column_ref[...] = column.reshape(octets)
    lane_pair = iota((slots, pairs), 1)
    sel = jnp.where(lane_pair // NBR == iota((slots, pairs), 0), 1.0, 0.0)
    limit = mm(count_ref[...].astype(f32).astype(bf16), sel.astype(bf16))
    order = (iota((1, pairs), 1) % NBR).astype(f32)
    live_ref[...] = jnp.where(order < limit, 1.0, 0.0).reshape(octets)

    zrow = zrow_ref[me]
    kcol = krow_ref[...]
    for j in range(planes):
        q = kcol[:, 0:1] + zrow[j : j + 1, 3:4] + kx_ref[0:1, :]
        scale = kcol[:, 1:2] * zrow[j : j + 1, 4:5] * kx_ref[1:2, :]
        green = (coulomb_scale * 4.0 * math.pi) * jnp.exp(-0.5 * smearing * smearing * q)
        green = green * scale / (q + 1.0 / (screen * screen))
        green_ref[j * length_y : (j + 1) * length_y] = jnp.where(q == 0.0, 0.0, green)
    plane_ref[...] = jnp.zeros(plane_ref.shape, f32)
    for z in range(size_z):
        lane = (iota((1, LANES), 1) + (z * cells_z * CELL - 1)).astype(f32)
        turns = zrow[:, 0:1] * lane
        turns = turns - length_z * jnp.floor(turns * (1.0 / length_z))
        angle = (turns - 0.5 * length_z) * (2.0 * math.pi / length_z)
        ztab_ref[z] = -jnp.cos(angle) * zrow[:, 1:2] - jnp.sin(angle) * zrow[:, 2:3]

    for r in range(rounds):
        pl.semaphore_wait(entered.at[r], close_count)
        if r + 1 < rounds:
            greet(entered.at[r + 1])
    for offset in offsets[close_count:]:
        atom_copy(index_of(offset, sizes), moved(offset, 1), me).start()
    for offset in offsets[:close_count]:
        origin = moved(offset, -1)
        atom_copy(index_of(offset, sizes), origin, index_of(origin, sizes)).wait()

    lane4 = iota((4, LANES), 1)
    for x in range(cells_x + 2):
        for pair_y in range(wide_y // 2):
            halves = []
            for y in (2 * pair_y, 2 * pair_y + 1):
                spots, locals_ = [], []
                for at, axis in ((x, 0), (y, 1)):
                    size = cells[axis]
                    if at == 0:
                        spots.append(lax.rem(here[axis] + sizes[axis] - 1, sizes[axis]))
                        locals_.append(size - 1)
                    elif at == size + 1:
                        spots.append(lax.rem(here[axis] + 1, sizes[axis]))
                        locals_.append(0)
                    else:
                        spots.append(here[axis])
                        locals_.append(at - 1)
                column = locals_[0] * cells_y + locals_[1]
                start_lane = column * run
                block = pl.ds(start_lane // LANES * LANES, LANES)
                odd = start_lane % LANES != 0
                pieces = []
                for step_z in (0, 1, size_z - 1):
                    origin = index_of(
                        (spots[0], spots[1], lax.rem(here[2] + step_z, size_z)), sizes
                    )
                    piece = all_ref[origin, :, block]
                    if (step_z == 0) == odd:
                        piece = pltpu.roll(piece, run, 1)
                    pieces.append(piece)
                line = jnp.where(
                    lane4 < run, pieces[0], jnp.where(lane4 < run + slots, pieces[1], pieces[2])
                )
                halves.append(line)
                if 1 <= x <= cells_x and 1 <= y <= cells_y:
                    mine_ref[column] = jnp.concatenate([line, line], axis=0)
            line_ref[x * (wide_y // 2) + pair_y] = jnp.concatenate(halves, axis=0)

    sub8 = iota((slots, LANES), 0)
    row_d = iota((slots, 1), 0)
    box = jnp.where(
        row_d == 0,
        float(length_x),
        jnp.where(row_d == 1, float(length_y), float(length_z)),
    )
    box_inv = 1.0 / box
    rates = jnp.zeros((rates_ref.shape[0], 1), f32)
    for k in range(rates_ref.shape[0]):
        rates = jnp.where(iota(rates.shape, 0) == k, rates_ref[k], rates)
    sub_y = sub8 // 4

    def geometry(octet, carry):
        for r in range(8):
            place_cell(octet * 8 + r, octet, r)
        return carry

    def place_cell(c, octet, r):
        cz = lax.rem(c, cells_z)
        cxy = c // cells_z
        cx = cxy // cells_y
        for chunk in range(pairs // LANES):
            part = pl.ds(chunk * LANES, LANES)
            spot = jnp.broadcast_to(zlane_ref[octet, r : r + 1, part], (slots, LANES))
            column = jnp.broadcast_to(column_ref[octet, r : r + 1, part], (slots, LANES)) - sub_y
            live = live_ref[octet, r : r + 1, part]
            which = which_ref[octet, r : r + 1, part]
            found = jnp.zeros((slots, LANES), f32)
            for dx in range(3):
                for pair_y in range(wide_y // 2):
                    table = line_ref[(cx + dx) * (wide_y // 2) + pair_y]
                    picked = lane_pick(table, spot)
                    found = jnp.where(column == dx * wide_y + 2 * pair_y, picked, found)
            found = found + pltpu.roll(found, 4, 0)
            own_spot = cz * slots + (lane8 + chunk * LANES) // NBR
            displace = found - lane_pick(mine_ref[cxy], own_spot)
            displace = displace - box * jnp.floor(displace * box_inv + 0.5)
            scaled = jnp.where(row_d < 3, displace * (1.0 / CELL), 0.0)
            square = jnp.sum(scaled * scaled, axis=0, keepdims=True)
            basis_ref[c, :, part] = jnp.exp(-square * rates)
            reach = jnp.where(row_d == 3, 1.0, scaled) * live
            reach_ref[c, :, part] = jnp.where(row_d == 4, which, reach)

    lax.fori_loop(0, cell_count // 8, geometry, 0, unroll=2)

    for copy in copies:
        copy.wait()
    for x in range(cells_x + 2):
        for y in range(wide_y):
            if 1 <= x <= cells_x and 1 <= y <= cells_y:
                blocks = [
                    near_ref[x, y, 0:1],
                    feat_ref[x - 1, y - 1],
                    near_ref[x, y, cells_z + 1 :],
                ]
            else:
                blocks = [near_ref[x, y]]
            line = [b.astype(f32).reshape(b.shape[0] * slots, channels) for b in blocks]
            line = jnp.concatenate(line, axis=0).astype(bf16)
            sent_ref[x * wide_y + y] = mm(line, wn_ref[...]).astype(bf16).astype(f32) * 0.5

    hot_rows = 27 * slots
    even_rows = hot_rows // 16 * 16
    hot_ids = iota((even_rows, 1), 0).astype(f32).astype(bf16)
    last_ids = (iota((hot_rows - even_rows, 1), 0) + even_rows).astype(f32)
    wr_rows = wr_ref[...].astype(f32) * 0.5
    sel_tile = jnp.concatenate([sel, sel], axis=0).astype(bf16)
    sub_h = iota((slots, half_pairs), 0)
    slot_h = iota((slots, half_pairs), 1) // NBR
    in_low = slot_h == sub_h
    in_high = slot_h == sub_h - slots // 2

    def pair_step(step, carry):
        rows = []
        for u in range(STEP_CELLS):
            c = step * STEP_CELLS + u
            cz = lax.rem(c, cells_z)
            cxy = c // cells_z
            cy = lax.rem(cxy, cells_y)
            cx = cxy // cells_y
            at = pl.ds(pl.multiple_of(cz * slots, slots), 3 * slots)
            mine = pl.ds(pl.multiple_of(c * slots, slots), slots)
            parts = []
            for dx in range(3):
                for dy in range(3):
                    parts.append(sent_ref[(cx + dx) * wide_y + cy + dy, at, :])
            parts += [wr_rows, own_ref[0, mine, :], own_ref[1, mine, :]]
            table = jnp.concatenate(parts, axis=0).astype(bf16).T
            which = reach_ref[c, 4:5, :]
            hot = jnp.where(
                hot_ids == which.astype(bf16), jnp.asarray(1.0, bf16), jnp.asarray(0.0, bf16)
            )
            last = jnp.where(last_ids == which, 1.0, 0.0)
            tile = jnp.concatenate([last, basis_ref[c]], axis=0).astype(bf16)
            rhs = jnp.concatenate([hot, tile, sel_tile], axis=0)
            latent = silu_of_half(mm(table, rhs)).T
            rows.append(jnp.concatenate([latent[:half_pairs], latent[half_pairs:]], axis=1))
        second = silu_of_half(mm(jnp.concatenate(rows, axis=0), bd1_ref[...]))
        third = silu_of_half(mm(second, bd2_ref[...]))
        for u in range(STEP_CELLS):
            c = step * STEP_CELLS + u
            mine = pl.ds(pl.multiple_of(c * slots, slots), slots)
            weights = []
            for r in (3, 0, 1, 2):
                low = reach_ref[c, r : r + 1, 0:half_pairs]
                high = reach_ref[c, r : r + 1, half_pairs:]
                full = jnp.where(in_low, low, jnp.where(in_high, high, 0.0))
                if r == 3:
                    weights.append(full)
                else:
                    full_hi = full.astype(bf16).astype(f32)
                    weights += [full_hi, full - full_hi]
            weights = jnp.concatenate(weights, axis=0).astype(bf16)
            sums = mm(weights, third[u * half_pairs : (u + 1) * half_pairs])
            rest = []
            for r in range(7):
                block = sums[r * slots : (r + 1) * slots]
                rest.append(
                    jnp.where(row_d < slots // 2, block[:, :channels], block[:, channels:])
                )
            msg_ref[mine, :] = rest[0] * (1.0 / NBR)
            for d in range(3):
                vec_ref[d, mine, :] = rest[1 + 2 * d] + rest[2 + 2 * d]
        return carry

    lanes = size_z * atom_count
    body_y = win_y - 8

    def spread(turn, carry):
        gx = lax.rem(here[0] + size_x - turn // size_y, size_x)
        gy = lax.rem(here[1] + size_y - lax.rem(turn, size_y), size_y)
        g = gx * size_y + gy
        base = g * size_z
        step_x, step_y = turn // size_y, lax.rem(turn, size_y)
        far_group = jnp.logical_or(
            jnp.logical_and(step_x > 1, step_x < size_x - 1),
            jnp.logical_and(step_y > 1, step_y < size_y - 1),
        )
        for z in range(size_z):
            gz = lax.rem(here[2] + size_z - z, size_z)
            copy = atom_copy(turn * size_z + z, (gx, gy, gz), base + gz)
            if z in (0, 1, size_z - 1):
                pl.when(far_group)(copy.wait)
            else:
                copy.wait()
        atoms = jnp.concatenate([all_ref[base + i] for i in range(size_z)], axis=1)
        whole = jnp.floor(atoms)
        f = atoms - whole
        sq = f * f
        cube = sq * f
        rem = 1.0 - f
        taps = [
            rem * rem * rem * (1.0 / 6.0),
            (3.0 * cube - 6.0 * sq + 4.0) * (1.0 / 6.0),
            (-3.0 * cube + 3.0 * sq + 3.0 * f + 1.0) * (1.0 / 6.0),
            cube * (1.0 / 6.0),
        ]
        for t in range(4):
            taps_ref[t] = taps[t]
        taps_ref[4] = whole
        first_x = (gx * (cells_x * CELL)).astype(f32)
        first_y = (gy * (cells_y * CELL)).astype(f32)
        tiles = win_x // 16

        def packed(row):
            wide = jnp.broadcast_to(row, (16, lanes))
            hi = wide.astype(bf16)
            return [hi, (wide - hi.astype(f32)).astype(bf16)]

        start_x = packed(taps_ref[4, 0:1, :] - first_x)[0]
        off_x = [(iota((16, 1), 0) + 16 * i).astype(f32).astype(bf16) - start_x for i in range(tiles)]
        none = jnp.zeros((16, lanes), bf16)
        x_hi = [none] * tiles
        x_lo = [none] * tiles
        for t in range(4):
            t_hi, t_lo = packed(taps_ref[t, 0:1, :])
            for i in range(tiles):
                hit = off_x[i] == jnp.asarray(t, bf16)
                x_hi[i] = jnp.where(hit, t_hi, x_hi[i])
                x_lo[i] = jnp.where(hit, t_lo, x_lo[i])
        row_y = iota((win_y, 1), 0)
        row_y = jnp.where(row_y < body_y + 4, row_y, row_y - 4).astype(f32)
        off_y = row_y - (taps_ref[4, 1:2, :] - first_y)
        rows_y = jnp.zeros((win_y, lanes), f32)
        for t in range(4):
            rows_y = jnp.where(off_y == float(t), taps_ref[t, 1:2, :], rows_y)
        waves = []
        for z in range(size_z):
            table = ztab_ref[z]
            for chunk in range(atom_count // LANES):
                part = slice(z * atom_count + chunk * LANES, z * atom_count + (chunk + 1) * LANES)
                spot = (taps_ref[4, 2:3, part] - float(z * cells_z * CELL)).astype(i32)
                spot = jnp.broadcast_to(spot, table.shape)
                wave = None
                for t in range(4):
                    term = lane_pick(table, spot + t) * taps_ref[t, 2:3, part]
                    wave = term if wave is None else wave + term
                waves.append(wave)
        wave = jnp.concatenate(waves, axis=1)
        wave_ref[g] = wave
        ys_ref[g] = rows_y
        rows_x = jnp.concatenate(x_hi + x_lo, axis=0)
        xs_ref[g] = rows_x
        scaled_ref[...] = wave * atoms[3:4]
        sub_low = iota((8, 1), 0) < 4
        left = [rows_y[:body_y] * scaled_ref[j : j + 1, :] for j in range(planes)]
        for j in range(0, planes, 2):
            both = jnp.where(sub_low, scaled_ref[j : j + 1, :], scaled_ref[j + 1 : j + 2, :])
            left.append(rows_y[body_y:] * both)
        left = jnp.concatenate(left, axis=0)
        l_hi, l_lo = two_pieces(left)
        res = mm_nt(l_hi, rows_x) + mm_nt(l_lo, rows_x)
        per_block = LANES // (2 * win_x)
        res = jnp.concatenate([res, jnp.zeros((res.shape[0], LANES - 2 * win_x), f32)], axis=1)
        res = pltpu.roll(res, lax.rem(gx, per_block) * (2 * win_x), 1)
        rows = pl.ds(pl.multiple_of(gy * win_y, 8), win_y)
        for j in range(planes):
            ends = res[planes * body_y + j // 2 * 8 : planes * body_y + j // 2 * 8 + 8]
            ends = jnp.where(sub_low if j % 2 == 0 else ~sub_low, ends, 0.0)
            body = res[j * body_y : (j + 1) * body_y]
            plane_ref[gx // per_block, j, rows, :] += jnp.concatenate([body, ends], axis=0)
        return carry

    lax.fori_loop(0, size_x * size_y, spread, 0)

    spectrum = None
    for block in range(plane_ref.shape[0]):
        for j in range(0, planes, 2):
            p_hi, p_lo = two_pieces(
                jnp.concatenate([plane_ref[block, j], plane_ref[block, j + 1]], axis=1)
            )
            both = mm(by_ref[0], p_hi) + mm(by_ref[0], p_lo) + mm(by_ref[1], p_hi)
            along_ref[j * length_y : (j + 1) * length_y, :] = both[:, :LANES]
            along_ref[(j + 1) * length_y : (j + 2) * length_y, :] = both[:, LANES:]
        a_hi, a_lo = two_pieces(along_ref[...])
        bxt_h = bxt_h_ref[block]
        part = mm(jnp.concatenate([a_hi, a_lo], axis=1), jnp.concatenate([bxt_h, bxt_h], axis=0))
        part = part + mm(a_hi, bxt_l_ref[block])
        spectrum = part if spectrum is None else spectrum + part
    s_hi, s_lo = two_pieces(spectrum * green_ref[...])
    lane_x = iota((1, 2 * LANES), 1) % (2 * win_x) < win_x
    for gx in range(0, size_x, 2):
        cols = slice(gx * LANES, (gx + 2) * LANES)
        back = (
            mm(s_hi, bxq_h_ref[:, cols]) + mm(s_lo, bxq_h_ref[:, cols]) + mm(s_hi, bxq_l_ref[:, cols])
        )
        b_hi, b_lo = two_pieces(back)
        for j in range(planes):
            rows = slice(j * length_y, (j + 1) * length_y)
            value = mm(
                byt_ref[...], jnp.concatenate([b_hi[rows], b_lo[rows], b_hi[rows]], axis=0)
            )
            v_hi = value.astype(bf16).astype(f32)
            value = jnp.where(lane_x, v_hi, value - v_hi)
            field_ref[gx, j] = value[:, :LANES]
            field_ref[gx + 1, j] = value[:, LANES:]

    def part_copy(o, peer):
        return pltpu.make_async_remote_copy(
            src_ref=part_ref.at[index_of(peer, sizes)],
            dst_ref=held_ref.at[o],
            send_sem=psend.at[o],
            recv_sem=precv.at[o],
            device_id=peer,
            device_id_type=pl.DeviceIdType.MESH,
        )

    def sample(g, carry):
        gx = g // size_y
        gy = lax.rem(g, size_y)
        rows = pl.ds(pl.multiple_of(gy * win_y, 8), win_y)
        planes_here = [field_ref[gx, j, rows, :] for j in range(planes)]
        sub_low = iota((8, 1), 0) < 4
        field = [block[:body_y] for block in planes_here]
        for j in range(0, planes, 2):
            field.append(
                jnp.where(sub_low, planes_here[j][body_y:], planes_here[j + 1][body_y:])
            )
        field = jnp.concatenate(field, axis=0)
        x_hi = xs_ref[g, 0:win_x]
        x_lo = xs_ref[g, win_x:]
        stack = [x_hi, x_hi, x_lo, x_lo] + [jnp.zeros_like(x_hi)] * (LANES // win_x - 4)
        values = mm(field.astype(bf16), jnp.concatenate(stack, axis=0))
        body = None
        ends = None
        for j in range(planes):
            term = values[j * body_y : (j + 1) * body_y] * wave_ref[g, j : j + 1, :]
            body = term if body is None else body + term
        for j in range(0, planes, 2):
            at = planes * body_y + j // 2 * 8
            both = jnp.where(sub_low, wave_ref[g, j : j + 1, :], wave_ref[g, j + 1 : j + 2, :])
            term = values[at : at + 8] * both
            ends = term if ends is None else ends + term
        mixed = jnp.concatenate([body, ends], axis=0)
        line = jnp.sum(mixed * ys_ref[g], axis=0, keepdims=True)
        for i in range(size_z):
            part_ref[g * size_z + i] = line[:, i * atom_count : (i + 1) * atom_count]
        return carry

    lax.fori_loop(0, size_x * size_y, sample, 0, unroll=4)

    for offset in offsets:
        part_copy(index_of(offset, sizes), moved(offset, 1)).start()

    lax.fori_loop(0, cell_count // STEP_CELLS, pair_step, 0)

    wv_twice = jnp.concatenate([wv_ref[...], wv_ref[...]], axis=0)
    invariant = None
    for d in range(3):
        vector = mm(jnp.concatenate(two_pieces(vec_ref[d]), axis=1), wv_twice)
        vector = vector * (1.0 / math.sqrt(NBR))
        part = vector * vector
        invariant = part if invariant is None else invariant + part
    update = (msg_ref[...] + invariant).astype(bf16)
    out_ref[...] = (hidden_ref[...].astype(f32) + mm(update, wo_ref[...])).astype(bf16)

    for offset in offsets:
        part_copy(index_of(offset, sizes), moved(offset, 1)).wait()
    held_ref[0] = part_ref[me]
    total = jnp.sum(held_ref[...], axis=0)
    rows = LANES // slots
    spot = iota((rows, LANES), 0) * slots + lax.rem(iota((rows, LANES), 1), slots)
    for chunk in range(atom_count // LANES):
        line = jnp.broadcast_to(total[:, chunk * LANES : (chunk + 1) * LANES], (rows, LANES))
        site_ref[chunk * rows : (chunk + 1) * rows, :] = lane_pick(line, spot)[:, :slots]


def staged_kernel(*args):
    count = args[7]
    layer_kernel(*args[:7], args[8 : 8 + count], *args[8 + count :])


def shards(
    features,
    positions,
    grid_anchor,
    species,
    neighbours,
    neighbour_count,
    w_self,
    w_neighbour,
    w_radial,
    radial_rates,
    w_pair1,
    w_pair2,
    w_vector,
    w_out,
    w_charge,
    species_charge,
):
    cells_x, cells_y, cells_z, slot_count, channels = features.shape
    cells = (cells_x, cells_y, cells_z)
    cell_count = cells_x * cells_y * cells_z
    atom_count = cell_count * slot_count
    sizes = tuple(lax.axis_size(a) for a in AXES)
    devices = sizes[0] * sizes[1] * sizes[2]
    lengths = tuple(c * s * CELL for c, s in zip(cells, sizes))
    length_x, length_y, length_z = lengths
    screen = 2 * cells_y * CELL
    pairs = slot_count * NBR

    share = length_z // 2 // devices
    planes = 2 * share
    win_x = -(-(cells_x * CELL + 4) // 16) * 16
    win_y = cells_y * CELL + 8
    assert 2 * cells_z * slot_count == LANES and cells_y % 2 == 0
    assert LANES % (4 * win_x) == 0 and cells_z * CELL + 4 <= LANES
    all_modes = np.arange(length_z // 2)
    table_k = np.stack([all_modes, all_modes], axis=1)
    phase_c = np.stack([np.ones_like(all_modes), np.zeros_like(all_modes)], axis=1)
    table_k[0, 1] = length_z // 2
    phase_c[0, 1] = 1
    table_k = table_k.reshape(devices, planes)
    phase_c = phase_c.reshape(devices, planes).astype(np.float64)
    basis_x, modes_x = trig_basis(length_x)
    basis_y, modes_y = trig_basis(length_y)
    qx, sx = axis_terms(modes_x, length_x)
    qy, sy = axis_terms(modes_y, length_y)
    qz, sz = axis_terms(table_k, length_z)
    krow = np.stack([qy, sy], axis=1).astype(np.float32)
    zrow = np.stack([table_k, phase_c, 1.0 - phase_c, qz, sz], axis=2)
    plane_rows = -(-planes // 8) * 8
    zrow = np.concatenate([zrow, np.ones((devices, plane_rows - planes, 5))], axis=1)
    zrow = zrow.astype(np.float32)
    kx = np.stack([qx, sx]).astype(np.float32)
    grid_x, grid_y = cells_x * CELL, cells_y * CELL
    row_y = np.arange(win_y)
    row_y = np.where(row_y < grid_y + 4, row_y, row_y - 4)
    at_y = np.concatenate([(row_y + g * grid_y - 1) % length_y for g in range(sizes[1])])
    by = basis_y[:, at_y]
    per_block = LANES // (2 * win_x)
    blocks = -(-sizes[0] // per_block)
    forward = np.zeros((blocks, LANES, length_x))
    backward = np.zeros((length_x, sizes[0] * LANES))
    for g in range(sizes[0]):
        cols = basis_x[:, (np.arange(win_x) + g * grid_x - 1) % length_x]
        at = g % per_block * 2 * win_x
        forward[g // per_block, at : at + 2 * win_x] = np.concatenate([cols, cols], axis=1).T
        backward[:, g * LANES : g * LANES + 4 * win_x] = np.concatenate([cols] * 4, axis=1)
    tables = [jnp.asarray(zrow), jnp.asarray(krow), jnp.asarray(kx)]
    by_hi, by_lo = host_pieces(by)
    tables.append(np.stack([by_hi, by_lo]))
    tables.append(np.concatenate([by_hi.T, by_hi.T, by_lo.T], axis=1))
    for table in (forward, backward):
        tables += host_pieces(table)
    tables = [jnp.asarray(t) for t in tables]

    operands = (
        features,
        features.reshape(atom_count, channels),
        positions.reshape(cell_count, 3 * slot_count),
        species.reshape(cell_count, slot_count),
        neighbours.reshape(cell_count, pairs),
        neighbour_count.reshape(cell_count, slot_count),
        w_self,
        w_neighbour,
        w_radial,
        radial_rates,
        w_pair1,
        w_pair2,
        w_vector,
        w_out,
        w_charge,
        species_charge,
        *tables,
    )
    vmem = pl.BlockSpec(memory_space=pltpu.VMEM)
    dma = pltpu.SemaphoreType.DMA
    groups = sizes[0] * sizes[1]
    lanes = sizes[2] * atom_count
    columns = (cells_x + 2) * (cells_y + 2)
    updated, site_potential = pl.pallas_call(
        functools.partial(
            staged_kernel, sizes, cells, lengths, screen, planes, win_x, win_y, len(operands)
        ),
        out_shape=(
            jax.ShapeDtypeStruct((atom_count, channels), bf16),
            jax.ShapeDtypeStruct((cell_count, slot_count), f32),
        ),
        in_specs=[pl.BlockSpec(memory_space=pl.ANY)] * len(operands),
        out_specs=(vmem, vmem),
        scratch_shapes=[
            pltpu.VMEM((4, atom_count), f32),
            pltpu.VMEM((devices, 4, atom_count), f32),
            pltpu.VMEM(tuple(c + 2 for c in cells) + (slot_count, channels), bf16),
            pltpu.VMEM((columns, (cells_z + 2) * slot_count, channels), f32),
            pltpu.VMEM((2, atom_count, channels), f32),
            pltpu.VMEM((cell_count // 8, 8, pairs), f32),
            pltpu.VMEM((cell_count // 8, 8, pairs), i32),
            pltpu.VMEM((cell_count // 8, 8, pairs), i32),
            pltpu.VMEM((cell_count // 8, 8, pairs), f32),
            pltpu.VMEM((planes * length_y, length_x), f32),
            pltpu.VMEM((columns // 2, 8, LANES), f32),
            pltpu.VMEM((cells_x * cells_y, 8, LANES), f32),
            pltpu.VMEM((cell_count, 8, pairs), f32),
            pltpu.VMEM((cell_count, 8, pairs), f32),
            pltpu.VMEM((sizes[2], plane_rows, LANES), f32),
            pltpu.VMEM((blocks, planes, sizes[1] * win_y, LANES), f32),
            pltpu.VMEM((planes * length_y, LANES), f32),
            pltpu.VMEM((sizes[0], planes, sizes[1] * win_y, LANES), f32),
            pltpu.VMEM((groups, plane_rows, lanes), f32),
            pltpu.VMEM((5, 4, lanes), f32),
            pltpu.VMEM((plane_rows, lanes), f32),
            pltpu.VMEM((groups, 2 * win_x, lanes), bf16),
            pltpu.VMEM((groups, win_y, lanes), f32),
            pltpu.VMEM((devices, 1, atom_count), f32),
            pltpu.VMEM((devices, 1, atom_count), f32),
            pltpu.VMEM((atom_count, channels), f32),
            pltpu.VMEM((3, atom_count, channels), f32),
            pltpu.VMEM((2 * channels, 2 * channels), bf16),
            pltpu.VMEM((2 * channels, 2 * channels), bf16),
            dma((devices,)),
            dma((devices,)),
            dma((27,)),
            dma((27,)),
            dma((devices,)),
            dma((devices,)),
            pltpu.SemaphoreType.REGULAR((max(max(size // 2 for size in sizes) - 1, 1),)),
            dma((len(operands),)),
        ]
        + [
            (pltpu.SMEM if a is radial_rates or a is species_charge else pltpu.VMEM)(
                a.shape, a.dtype
            )
            for a in operands
        ],
        name="fused_layer",
        compiler_params=pltpu.CompilerParams(
            has_side_effects=True, collective_id=0, vmem_limit_bytes=VMEM_BYTES
        ),
    )(*operands)
    return (
        updated.reshape(features.shape),
        site_potential.reshape(cells_x, cells_y, cells_z, slot_count),
    )


def solution(mesh):
    cells = P("gx", "gy", "gz", None)
    return jax.shard_map(
        shards,
        mesh=mesh,
        in_specs=(P("gx", "gy", "gz", None, None),) + (cells,) * 5 + (P(),) * 10,
        out_specs=(P("gx", "gy", "gz", None, None), cells),
        check_vma=False,
    )
```

```python
import functools
import math

import jax
import jax.numpy as jnp
import numpy as np
from jax import lax
from jax.experimental import pallas as pl
from jax.experimental.pallas import tpu as pltpu
from jax.sharding import PartitionSpec as P

NBR = 64
CELL = 8
LANES = 128
STEP_CELLS = 12
FIRST_LOADS = (2, 3, 1, 14, 15, 0)
VMEM_BYTES = 60 * 1024 * 1024
AXES = ("gx", "gy", "gz")

coulomb_scale = 0.25
smearing = 1.0
f32, bf16, i32 = jnp.float32, jnp.bfloat16, jnp.int32


def index_of(coords, sizes):
    return (coords[0] * sizes[1] + coords[1]) * sizes[2] + coords[2]


def iota(shape, axis):
    return lax.broadcasted_iota(i32, shape, axis)


def split_by(value, size):
    if size & (size - 1) == 0:
        shift = size.bit_length() - 1
        return lax.shift_right_logical(value, shift), value & (size - 1)
    high = jnp.floor((value.astype(f32) + 0.5) * (1.0 / size)).astype(i32)
    return high, value - high * size


def two_pieces(x):
    hi = x.astype(bf16)
    return hi, (x - hi.astype(f32)).astype(bf16)


def mm(a, b):
    return jnp.dot(a, b, preferred_element_type=f32)


def mm_nt(a, b):
    return lax.dot_general(a, b, (((1,), (1,)), ((), ())), preferred_element_type=f32)


def lane_pick(table, index):
    dims = lax.GatherDimensionNumbers(
        offset_dims=(),
        collapsed_slice_dims=(1,),
        start_index_map=(1,),
        operand_batching_dims=(0,),
        start_indices_batching_dims=(0,),
    )
    return lax.gather(
        table, index[..., None], dims, (1, 1), mode=lax.GatherScatterMode.PROMISE_IN_BOUNDS
    )


def silu_of_half(half):
    return (half + half * jnp.tanh(half)).astype(bf16)


def trig_basis(length):
    r = np.arange(length)
    rows = [np.cos(2 * np.pi * ((k * r) % length) / length) for k in range(length // 2 + 1)]
    rows += [np.sin(2 * np.pi * ((k * r) % length) / length) for k in range(1, length // 2)]
    modes = np.array(list(range(length // 2 + 1)) + list(range(1, length // 2)))
    return np.stack(rows), modes


def axis_terms(modes, length):
    wave = modes * (2.0 * np.pi / length)
    turn = np.exp(2j * np.pi * modes / length)
    modulus = np.abs(1 / 6 + 4 / 6 * turn + 1 / 6 * turn * turn) ** 2
    weight = np.where((modes == 0) | (2 * modes == length), 1.0, 2.0) / length
    return wave * wave, weight / modulus


def host_pieces(table):
    table = np.ascontiguousarray(table).astype(np.float32)
    hi = table.astype(jnp.bfloat16)
    lo = (table - hi.astype(np.float32)).astype(jnp.bfloat16)
    return hi, lo


def layer_kernel(
    sizes,
    cells,
    lengths,
    screen,
    planes,
    win_x,
    win_y,
    sources,
    out_ref,
    site_ref,
    atoms_ref,
    all_ref,
    near_ref,
    sent_ref,
    own_ref,
    which_ref,
    zlane_ref,
    column_ref,
    live_ref,
    green_ref,
    line_ref,
    mine_ref,
    basis_ref,
    reach_ref,
    ztab_ref,
    plane_ref,
    along_ref,
    field_ref,
    wave_ref,
    taps_ref,
    scaled_ref,
    xs_ref,
    ys_ref,
    part_ref,
    held_ref,
    msg_ref,
    vec_ref,
    bd1_ref,
    bd2_ref,
    asend,
    arecv,
    hsend,
    hrecv,
    psend,
    precv,
    entered,
    stage_sem,
    *staged,
):
    (
        feat_ref,
        hidden_ref,
        pos_ref,
        kind_ref,
        nbr_ref,
        count_ref,
        ws_ref,
        wn_ref,
        wr_ref,
        rates_ref,
        w1_ref,
        w2_ref,
        wv_ref,
        wo_ref,
        wc_ref,
        kinds_ref,
        zrow_ref,
        krow_ref,
        kx_ref,
        by_ref,
        byt_ref,
        bxt_h_ref,
        bxt_l_ref,
        bxq_h_ref,
        bxq_l_ref,
    ) = staged
    loads = [
        pltpu.make_async_copy(source, target, stage_sem.at[k])
        for k, (source, target) in enumerate(zip(sources, staged))
    ]
    for k in FIRST_LOADS:
        loads[k].start()
    size_x, size_y, size_z = sizes
    cells_x, cells_y, cells_z = cells
    length_x, length_y, length_z = lengths
    devices = size_x * size_y * size_z
    slots = feat_ref.shape[3]
    channels = feat_ref.shape[4]
    cell_count = cells_x * cells_y * cells_z
    atom_count = cell_count * slots
    pairs = slots * NBR
    half_pairs = pairs // 2
    run = cells_z * slots
    wide_y = cells_y + 2
    here = tuple(lax.axis_index(a) for a in AXES)
    me = index_of(here, sizes)

    offsets = [
        (a, b, c)
        for a in range(size_x)
        for b in range(size_y)
        for c in range(size_z)
        if (a, b, c) != (0, 0, 0)
    ]
    close = [
        all(step in (0, 1, size - 1) for step, size in zip(offset, sizes)) for offset in offsets
    ]
    offsets = [o for o, c in zip(offsets, close) if c] + [o for o, c in zip(offsets, close) if not c]
    close_count = sum(close)

    def moved(offset, sign):
        return tuple(
            lax.rem(at + (step if sign > 0 else size - step), size) if step else at
            for at, step, size in zip(here, offset, sizes)
        )

    def greet(semaphore):
        for offset in offsets[:close_count]:
            pl.semaphore_signal(
                semaphore, inc=1, device_id=moved(offset, 1), device_id_type=pl.DeviceIdType.MESH
            )

    barrier = pltpu.get_barrier_semaphore()
    greet(barrier)
    for k in range(len(loads)):
        if k not in FIRST_LOADS:
            loads[k].start()
    for k in FIRST_LOADS:
        loads[k].wait()

    pad_rows = jnp.zeros((LANES - cell_count, 1), f32)
    kinds = kind_ref[...].astype(f32)
    turned = [
        jnp.concatenate(
            [block, jnp.zeros((LANES - cell_count, block.shape[1]), f32)], axis=0
        ).T
        for block in (pos_ref[...], kinds)
    ]
    lane8 = iota((slots, LANES), 1)
    diagonal = (lane8 % slots) == iota((slots, LANES), 0)
    per_chunk = LANES // slots
    wc_rows = jnp.broadcast_to(wc_ref[...].reshape(1, channels), (slots, channels))
    readout = mm_nt(wc_rows, hidden_ref[...])

    def lined(block, chunk):
        picked = lane_pick(block, lane8 // slots + chunk * per_chunk)
        return jnp.sum(jnp.where(diagonal, picked, 0.0), axis=0, keepdims=True)

    for chunk in range(atom_count // LANES):
        where_to = slice(chunk * LANES, (chunk + 1) * LANES)
        for d in range(3):
            atoms_ref[d : d + 1, where_to] = lined(turned[0][d * slots : (d + 1) * slots], chunk)
        kind = lined(turned[1], chunk)
        charge = readout[0:1, where_to]
        for k in range(kinds_ref.shape[0]):
            charge = charge + jnp.where(kind == float(k), kinds_ref[k], 0.0)
        atoms_ref[3:4, where_to] = charge

    def atom_copy(at, peer, slot):
        return pltpu.make_async_remote_copy(
            src_ref=atoms_ref,
            dst_ref=all_ref.at[slot],
            send_sem=asend.at[at],
            recv_sem=arecv.at[at],
            device_id=peer,
            device_id_type=pl.DeviceIdType.MESH,
        )

    copies = []
    for shift in range(27):
        step = (shift // 9 - 1, shift // 3 % 3 - 1, shift % 3 - 1)
        if step == (0, 0, 0):
            continue
        source, target, peer = [], [], []
        for axis in range(3):
            size = cells[axis]
            if step[axis] == 0:
                source.append(pl.ds(0, size))
                target.append(pl.ds(1, size))
                peer.append(here[axis])
            elif step[axis] > 0:
                source.append(pl.ds(size - 1, 1))
                target.append(pl.ds(0, 1))
                peer.append(lax.rem(here[axis] + 1, sizes[axis]))
            else:
                source.append(pl.ds(0, 1))
                target.append(pl.ds(size + 1, 1))
                peer.append(lax.rem(here[axis] + sizes[axis] - 1, sizes[axis]))
        copies.append(
            pltpu.make_async_remote_copy(
                src_ref=feat_ref.at[tuple(source)],
                dst_ref=near_ref.at[tuple(target)],
                send_sem=hsend.at[shift],
                recv_sem=hrecv.at[shift],
                device_id=tuple(peer),
                device_id_type=pl.DeviceIdType.MESH,
            )
        )
    pl.semaphore_wait(barrier, close_count)
    for offset in offsets[:close_count]:
        atom_copy(index_of(offset, sizes), moved(offset, 1), me).start()
    rounds = max(size // 2 for size in sizes) - 1
    if rounds > 0:
        greet(entered.at[0])
    for copy in copies:
        copy.start()
    all_ref[me] = atoms_ref[...]

    for k in range(len(loads)):
        if k not in FIRST_LOADS:
            loads[k].wait()

    own = mm(hidden_ref[...], ws_ref[...]) * 0.5
    own_hi = own.astype(bf16).astype(f32)
    own_ref[0] = own_hi
    own_ref[1] = (own - own_hi).astype(bf16).astype(f32)

    no_block = jnp.zeros((channels, channels), bf16)
    for ref, target in ((w1_ref, bd1_ref), (w2_ref, bd2_ref)):
        weight = ref[...] * jnp.asarray(0.5, bf16)
        target[0:channels, 0:channels] = weight
        target[0:channels, channels:] = no_block
        target[channels:, 0:channels] = no_block
        target[channels:, channels:] = weight

    listed = nbr_ref[...]
    cell_id, slot_id = split_by(listed, slots)
    xy_id, z_id = split_by(cell_id, cells_z * size_z)
    x_id, y_id = split_by(xy_id, cells_y * size_y)
    row_xy, row_z = split_by(iota((cell_count, 1), 0), cells_z)
    row_x, row_y = split_by(row_xy, cells_y)
    steps = []
    for ids, local, axis in ((x_id, row_x, 0), (y_id, row_y, 1), (z_id, row_z, 2)):
        total = cells[axis] * sizes[axis]
        gap = ids - (local + here[axis] * cells[axis])
        gap = jnp.where(gap > 1, gap - total, gap)
        steps.append(jnp.where(gap < -1, gap + total, gap))
    which = ((steps[0] + 1) * 3 + steps[1] + 1) * (3 * slots) + (steps[2] + 1) * slots + slot_id
    octets = which_ref.shape
    which_ref[...] = which.astype(f32).reshape(octets)
    zlane = ((row_z + steps[2]) * slots + slot_id) & (LANES - 1)
    zlane_ref[...] = zlane.reshape(octets)
    column = (steps[0] + 1) * wide_y + row_y + 1 + steps[1]
    column_ref[...] = column.reshape(octets)
    lane_pair = iota((slots, pairs), 1)
    sel = jnp.where(lane_pair // NBR == iota((slots, pairs), 0), 1.0, 0.0)
    limit = mm(count_ref[...].astype(f32).astype(bf16), sel.astype(bf16))
    order = (iota((1, pairs), 1) % NBR).astype(f32)
    live_ref[...] = jnp.where(order < limit, 1.0, 0.0).reshape(octets)

    zrow = zrow_ref[me]
    kcol = krow_ref[...]
    for j in range(planes):
        q = kcol[:, 0:1] + zrow[j : j + 1, 3:4] + kx_ref[0:1, :]
        scale = kcol[:, 1:2] * zrow[j : j + 1, 4:5] * kx_ref[1:2, :]
        green = (coulomb_scale * 4.0 * math.pi) * jnp.exp(-0.5 * smearing * smearing * q)
        green = green * scale / (q + 1.0 / (screen * screen))
        green_ref[j * length_y : (j + 1) * length_y] = jnp.where(q == 0.0, 0.0, green)
    plane_ref[...] = jnp.zeros(plane_ref.shape, f32)
    for z in range(size_z):
        lane = (iota((1, LANES), 1) + (z * cells_z * CELL - 1)).astype(f32)
        turns = zrow[:, 0:1] * lane
        turns = turns - length_z * jnp.floor(turns * (1.0 / length_z))
        angle = (turns - 0.5 * length_z) * (2.0 * math.pi / length_z)
        ztab_ref[z] = -jnp.cos(angle) * zrow[:, 1:2] - jnp.sin(angle) * zrow[:, 2:3]

    for r in range(rounds):
        pl.semaphore_wait(entered.at[r], close_count)
        if r + 1 < rounds:
            greet(entered.at[r + 1])
    for offset in offsets[close_count:]:
        atom_copy(index_of(offset, sizes), moved(offset, 1), me).start()
    for offset in offsets[:close_count]:
        origin = moved(offset, -1)
        atom_copy(index_of(offset, sizes), origin, index_of(origin, sizes)).wait()

    lane4 = iota((4, LANES), 1)
    for x in range(cells_x + 2):
        for pair_y in range(wide_y // 2):
            halves = []
            for y in (2 * pair_y, 2 * pair_y + 1):
                spots, locals_ = [], []
                for at, axis in ((x, 0), (y, 1)):
                    size = cells[axis]
                    if at == 0:
                        spots.append(lax.rem(here[axis] + sizes[axis] - 1, sizes[axis]))
                        locals_.append(size - 1)
                    elif at == size + 1:
                        spots.append(lax.rem(here[axis] + 1, sizes[axis]))
                        locals_.append(0)
                    else:
                        spots.append(here[axis])
                        locals_.append(at - 1)
                column = locals_[0] * cells_y + locals_[1]
                start_lane = column * run
                block = pl.ds(start_lane // LANES * LANES, LANES)
                odd = start_lane % LANES != 0
                pieces = []
                for step_z in (0, 1, size_z - 1):
                    origin = index_of(
                        (spots[0], spots[1], lax.rem(here[2] + step_z, size_z)), sizes
                    )
                    piece = all_ref[origin, :, block]
                    if (step_z == 0) == odd:
                        piece = pltpu.roll(piece, run, 1)
                    pieces.append(piece)
                line = jnp.where(
                    lane4 < run, pieces[0], jnp.where(lane4 < run + slots, pieces[1], pieces[2])
                )
                halves.append(line)
                if 1 <= x <= cells_x and 1 <= y <= cells_y:
                    mine_ref[column] = jnp.concatenate([line, line], axis=0)
            line_ref[x * (wide_y // 2) + pair_y] = jnp.concatenate(halves, axis=0)

    sub8 = iota((slots, LANES), 0)
    row_d = iota((slots, 1), 0)
    box = jnp.where(
        row_d == 0,
        float(length_x),
        jnp.where(row_d == 1, float(length_y), float(length_z)),
    )
    box_inv = 1.0 / box
    rates = jnp.zeros((rates_ref.shape[0], 1), f32)
    for k in range(rates_ref.shape[0]):
        rates = jnp.where(iota(rates.shape, 0) == k, rates_ref[k], rates)
    sub_y = sub8 // 4

    def geometry(octet, carry):
        for r in range(8):
            place_cell(octet * 8 + r, octet, r)
        return carry

    def place_cell(c, octet, r):
        cz = lax.rem(c, cells_z)
        cxy = c // cells_z
        cx = cxy // cells_y
        for chunk in range(pairs // LANES):
            part = pl.ds(chunk * LANES, LANES)
            spot = jnp.broadcast_to(zlane_ref[octet, r : r + 1, part], (slots, LANES))
            column = jnp.broadcast_to(column_ref[octet, r : r + 1, part], (slots, LANES)) - sub_y
            live = live_ref[octet, r : r + 1, part]
            which = which_ref[octet, r : r + 1, part]
            found = jnp.zeros((slots, LANES), f32)
            for dx in range(3):
                for pair_y in range(wide_y // 2):
                    table = line_ref[(cx + dx) * (wide_y // 2) + pair_y]
                    picked = lane_pick(table, spot)
                    found = jnp.where(column == dx * wide_y + 2 * pair_y, picked, found)
            found = found + pltpu.roll(found, 4, 0)
            own_spot = cz * slots + (lane8 + chunk * LANES) // NBR
            displace = found - lane_pick(mine_ref[cxy], own_spot)
            displace = displace - box * jnp.floor(displace * box_inv + 0.5)
            scaled = jnp.where(row_d < 3, displace * (1.0 / CELL), 0.0)
            square = jnp.sum(scaled * scaled, axis=0, keepdims=True)
            basis_ref[c, :, part] = jnp.exp(-square * rates)
            reach = jnp.where(row_d == 3, 1.0, scaled) * live
            reach_ref[c, :, part] = jnp.where(row_d == 4, which, reach)

    lax.fori_loop(0, cell_count // 8, geometry, 0, unroll=2)

    for copy in copies:
        copy.wait()
    for x in range(cells_x + 2):
        for y in range(wide_y):
            if 1 <= x <= cells_x and 1 <= y <= cells_y:
                blocks = [
                    near_ref[x, y, 0:1],
                    feat_ref[x - 1, y - 1],
                    near_ref[x, y, cells_z + 1 :],
                ]
            else:
                blocks = [near_ref[x, y]]
            line = [b.astype(f32).reshape(b.shape[0] * slots, channels) for b in blocks]
            line = jnp.concatenate(line, axis=0).astype(bf16)
            sent_ref[x * wide_y + y] = mm(line, wn_ref[...]).astype(bf16).astype(f32) * 0.5

    hot_rows = 27 * slots
    even_rows = hot_rows // 16 * 16
    hot_ids = iota((even_rows, 1), 0).astype(f32).astype(bf16)
    last_ids = (iota((hot_rows - even_rows, 1), 0) + even_rows).astype(f32)
    wr_rows = wr_ref[...].astype(f32) * 0.5
    sel_tile = jnp.concatenate([sel, sel], axis=0).astype(bf16)
    sub_h = iota((slots, half_pairs), 0)
    slot_h = iota((slots, half_pairs), 1) // NBR
    in_low = slot_h == sub_h
    in_high = slot_h == sub_h - slots // 2

    def pair_step(step, carry):
        rows = []
        for u in range(STEP_CELLS):
            c = step * STEP_CELLS + u
            cz = lax.rem(c, cells_z)
            cxy = c // cells_z
            cy = lax.rem(cxy, cells_y)
            cx = cxy // cells_y
            at = pl.ds(pl.multiple_of(cz * slots, slots), 3 * slots)
            mine = pl.ds(pl.multiple_of(c * slots, slots), slots)
            parts = []
            for dx in range(3):
                for dy in range(3):
                    parts.append(sent_ref[(cx + dx) * wide_y + cy + dy, at, :])
            parts += [wr_rows, own_ref[0, mine, :], own_ref[1, mine, :]]
            table = jnp.concatenate(parts, axis=0).astype(bf16).T
            which = reach_ref[c, 4:5, :]
            hot = jnp.where(
                hot_ids == which.astype(bf16), jnp.asarray(1.0, bf16), jnp.asarray(0.0, bf16)
            )
            last = jnp.where(last_ids == which, 1.0, 0.0)
            tile = jnp.concatenate([last, basis_ref[c]], axis=0).astype(bf16)
            rhs = jnp.concatenate([hot, tile, sel_tile], axis=0)
            latent = silu_of_half(mm(table, rhs)).T
            rows.append(jnp.concatenate([latent[:half_pairs], latent[half_pairs:]], axis=1))
        second = silu_of_half(mm(jnp.concatenate(rows, axis=0), bd1_ref[...]))
        third = silu_of_half(mm(second, bd2_ref[...]))
        for u in range(STEP_CELLS):
            c = step * STEP_CELLS + u
            mine = pl.ds(pl.multiple_of(c * slots, slots), slots)
            weights = []
            for r in (3, 0, 1, 2):
                low = reach_ref[c, r : r + 1, 0:half_pairs]
                high = reach_ref[c, r : r + 1, half_pairs:]
                full = jnp.where(in_low, low, jnp.where(in_high, high, 0.0))
                if r == 3:
                    weights.append(full)
                else:
                    full_hi = full.astype(bf16).astype(f32)
                    weights += [full_hi, full - full_hi]
            weights = jnp.concatenate(weights, axis=0).astype(bf16)
            sums = mm(weights, third[u * half_pairs : (u + 1) * half_pairs])
            rest = []
            for r in range(7):
                block = sums[r * slots : (r + 1) * slots]
                rest.append(
                    jnp.where(row_d < slots // 2, block[:, :channels], block[:, channels:])
                )
            msg_ref[mine, :] = rest[0] * (1.0 / NBR)
            for d in range(3):
                vec_ref[d, mine, :] = rest[1 + 2 * d] + rest[2 + 2 * d]
        return carry

    lanes = size_z * atom_count
    body_y = win_y - 8

    def spread(turn, carry):
        gx = lax.rem(here[0] + size_x - turn // size_y, size_x)
        gy = lax.rem(here[1] + size_y - lax.rem(turn, size_y), size_y)
        g = gx * size_y + gy
        base = g * size_z
        step_x, step_y = turn // size_y, lax.rem(turn, size_y)
        far_group = jnp.logical_or(
            jnp.logical_and(step_x > 1, step_x < size_x - 1),
            jnp.logical_and(step_y > 1, step_y < size_y - 1),
        )
        for z in range(size_z):
            gz = lax.rem(here[2] + size_z - z, size_z)
            copy = atom_copy(turn * size_z + z, (gx, gy, gz), base + gz)
            if z in (0, 1, size_z - 1):
                pl.when(far_group)(copy.wait)
            else:
                copy.wait()
        atoms = jnp.concatenate([all_ref[base + i] for i in range(size_z)], axis=1)
        whole = jnp.floor(atoms)
        f = atoms - whole
        sq = f * f
        cube = sq * f
        rem = 1.0 - f
        taps = [
            rem * rem * rem * (1.0 / 6.0),
            (3.0 * cube - 6.0 * sq + 4.0) * (1.0 / 6.0),
            (-3.0 * cube + 3.0 * sq + 3.0 * f + 1.0) * (1.0 / 6.0),
            cube * (1.0 / 6.0),
        ]
        for t in range(4):
            taps_ref[t] = taps[t]
        taps_ref[4] = whole
        first_x = (gx * (cells_x * CELL)).astype(f32)
        first_y = (gy * (cells_y * CELL)).astype(f32)
        tiles = win_x // 16

        def packed(row):
            wide = jnp.broadcast_to(row, (16, lanes))
            hi = wide.astype(bf16)
            return [hi, (wide - hi.astype(f32)).astype(bf16)]

        start_x = packed(taps_ref[4, 0:1, :] - first_x)[0]
        off_x = [(iota((16, 1), 0) + 16 * i).astype(f32).astype(bf16) - start_x for i in range(tiles)]
        none = jnp.zeros((16, lanes), bf16)
        x_hi = [none] * tiles
        x_lo = [none] * tiles
        for t in range(4):
            t_hi, t_lo = packed(taps_ref[t, 0:1, :])
            for i in range(tiles):
                hit = off_x[i] == jnp.asarray(t, bf16)
                x_hi[i] = jnp.where(hit, t_hi, x_hi[i])
                x_lo[i] = jnp.where(hit, t_lo, x_lo[i])
        row_y = iota((win_y, 1), 0)
        row_y = jnp.where(row_y < body_y + 4, row_y, row_y - 4).astype(f32)
        off_y = row_y - (taps_ref[4, 1:2, :] - first_y)
        rows_y = jnp.zeros((win_y, lanes), f32)
        for t in range(4):
            rows_y = jnp.where(off_y == float(t), taps_ref[t, 1:2, :], rows_y)
        waves = []
        for z in range(size_z):
            table = ztab_ref[z]
            for chunk in range(atom_count // LANES):
                part = slice(z * atom_count + chunk * LANES, z * atom_count + (chunk + 1) * LANES)
                spot = (taps_ref[4, 2:3, part] - float(z * cells_z * CELL)).astype(i32)
                spot = jnp.broadcast_to(spot, table.shape)
                wave = None
                for t in range(4):
                    term = lane_pick(table, spot + t) * taps_ref[t, 2:3, part]
                    wave = term if wave is None else wave + term
                waves.append(wave)
        wave = jnp.concatenate(waves, axis=1)
        wave_ref[g] = wave
        ys_ref[g] = rows_y
        rows_x = jnp.concatenate(x_hi + x_lo, axis=0)
        xs_ref[g] = rows_x
        scaled_ref[...] = wave * atoms[3:4]
        sub_low = iota((8, 1), 0) < 4
        left = [rows_y[:body_y] * scaled_ref[j : j + 1, :] for j in range(planes)]
        for j in range(0, planes, 2):
            both = jnp.where(sub_low, scaled_ref[j : j + 1, :], scaled_ref[j + 1 : j + 2, :])
            left.append(rows_y[body_y:] * both)
        left = jnp.concatenate(left, axis=0)
        l_hi, l_lo = two_pieces(left)
        res = mm_nt(l_hi, rows_x) + mm_nt(l_lo, rows_x)
        per_block = LANES // (2 * win_x)
        res = jnp.concatenate([res, jnp.zeros((res.shape[0], LANES - 2 * win_x), f32)], axis=1)
        res = pltpu.roll(res, lax.rem(gx, per_block) * (2 * win_x), 1)
        rows = pl.ds(pl.multiple_of(gy * win_y, 8), win_y)
        for j in range(planes):
            ends = res[planes * body_y + j // 2 * 8 : planes * body_y + j // 2 * 8 + 8]
            ends = jnp.where(sub_low if j % 2 == 0 else ~sub_low, ends, 0.0)
            body = res[j * body_y : (j + 1) * body_y]
            plane_ref[gx // per_block, j, rows, :] += jnp.concatenate([body, ends], axis=0)
        return carry

    lax.fori_loop(0, size_x * size_y, spread, 0)

    spectrum = None
    for block in range(plane_ref.shape[0]):
        for j in range(0, planes, 2):
            p_hi, p_lo = two_pieces(
                jnp.concatenate([plane_ref[block, j], plane_ref[block, j + 1]], axis=1)
            )
            both = mm(by_ref[0], p_hi) + mm(by_ref[0], p_lo) + mm(by_ref[1], p_hi)
            along_ref[j * length_y : (j + 1) * length_y, :] = both[:, :LANES]
            along_ref[(j + 1) * length_y : (j + 2) * length_y, :] = both[:, LANES:]
        a_hi, a_lo = two_pieces(along_ref[...])
        bxt_h = bxt_h_ref[block]
        part = mm(jnp.concatenate([a_hi, a_lo], axis=1), jnp.concatenate([bxt_h, bxt_h], axis=0))
        part = part + mm(a_hi, bxt_l_ref[block])
        spectrum = part if spectrum is None else spectrum + part
    s_hi, s_lo = two_pieces(spectrum * green_ref[...])
    lane_x = iota((1, 2 * LANES), 1) % (2 * win_x) < win_x
    for gx in range(0, size_x, 2):
        cols = slice(gx * LANES, (gx + 2) * LANES)
        back = (
            mm(s_hi, bxq_h_ref[:, cols]) + mm(s_lo, bxq_h_ref[:, cols]) + mm(s_hi, bxq_l_ref[:, cols])
        )
        b_hi, b_lo = two_pieces(back)
        for j in range(planes):
            rows = slice(j * length_y, (j + 1) * length_y)
            value = mm(
                byt_ref[...], jnp.concatenate([b_hi[rows], b_lo[rows], b_hi[rows]], axis=0)
            )
            v_hi = value.astype(bf16).astype(f32)
            value = jnp.where(lane_x, v_hi, value - v_hi)
            field_ref[gx, j] = value[:, :LANES]
            field_ref[gx + 1, j] = value[:, LANES:]

    def part_copy(o, peer):
        return pltpu.make_async_remote_copy(
            src_ref=part_ref.at[index_of(peer, sizes)],
            dst_ref=held_ref.at[o],
            send_sem=psend.at[o],
            recv_sem=precv.at[o],
            device_id=peer,
            device_id_type=pl.DeviceIdType.MESH,
        )

    def sample(g, carry):
        gx = g // size_y
        gy = lax.rem(g, size_y)
        rows = pl.ds(pl.multiple_of(gy * win_y, 8), win_y)
        planes_here = [field_ref[gx, j, rows, :] for j in range(planes)]
        sub_low = iota((8, 1), 0) < 4
        field = [block[:body_y] for block in planes_here]
        for j in range(0, planes, 2):
            field.append(
                jnp.where(sub_low, planes_here[j][body_y:], planes_here[j + 1][body_y:])
            )
        field = jnp.concatenate(field, axis=0)
        x_hi = xs_ref[g, 0:win_x]
        x_lo = xs_ref[g, win_x:]
        stack = [x_hi, x_hi, x_lo, x_lo] + [jnp.zeros_like(x_hi)] * (LANES // win_x - 4)
        values = mm(field.astype(bf16), jnp.concatenate(stack, axis=0))
        body = None
        ends = None
        for j in range(planes):
            term = values[j * body_y : (j + 1) * body_y] * wave_ref[g, j : j + 1, :]
            body = term if body is None else body + term
        for j in range(0, planes, 2):
            at = planes * body_y + j // 2 * 8
            both = jnp.where(sub_low, wave_ref[g, j : j + 1, :], wave_ref[g, j + 1 : j + 2, :])
            term = values[at : at + 8] * both
            ends = term if ends is None else ends + term
        mixed = jnp.concatenate([body, ends], axis=0)
        line = jnp.sum(mixed * ys_ref[g], axis=0, keepdims=True)
        for i in range(size_z):
            part_ref[g * size_z + i] = line[:, i * atom_count : (i + 1) * atom_count]
        return carry

    lax.fori_loop(0, size_x * size_y, sample, 0, unroll=8)

    for offset in offsets:
        part_copy(index_of(offset, sizes), moved(offset, 1)).start()

    lax.fori_loop(0, cell_count // STEP_CELLS, pair_step, 0)

    wv_twice = jnp.concatenate([wv_ref[...], wv_ref[...]], axis=0)
    invariant = None
    for d in range(3):
        vector = mm(jnp.concatenate(two_pieces(vec_ref[d]), axis=1), wv_twice)
        vector = vector * (1.0 / math.sqrt(NBR))
        part = vector * vector
        invariant = part if invariant is None else invariant + part
    update = (msg_ref[...] + invariant).astype(bf16)
    out_ref[...] = (hidden_ref[...].astype(f32) + mm(update, wo_ref[...])).astype(bf16)

    for offset in offsets:
        part_copy(index_of(offset, sizes), moved(offset, 1)).wait()
    held_ref[0] = part_ref[me]
    total = jnp.sum(held_ref[...], axis=0)
    rows = LANES // slots
    spot = iota((rows, LANES), 0) * slots + lax.rem(iota((rows, LANES), 1), slots)
    for chunk in range(atom_count // LANES):
        line = jnp.broadcast_to(total[:, chunk * LANES : (chunk + 1) * LANES], (rows, LANES))
        site_ref[chunk * rows : (chunk + 1) * rows, :] = lane_pick(line, spot)[:, :slots]


def staged_kernel(*args):
    count = args[7]
    layer_kernel(*args[:7], args[8 : 8 + count], *args[8 + count :])


def shards(
    features,
    positions,
    grid_anchor,
    species,
    neighbours,
    neighbour_count,
    w_self,
    w_neighbour,
    w_radial,
    radial_rates,
    w_pair1,
    w_pair2,
    w_vector,
    w_out,
    w_charge,
    species_charge,
):
    cells_x, cells_y, cells_z, slot_count, channels = features.shape
    cells = (cells_x, cells_y, cells_z)
    cell_count = cells_x * cells_y * cells_z
    atom_count = cell_count * slot_count
    sizes = tuple(lax.axis_size(a) for a in AXES)
    devices = sizes[0] * sizes[1] * sizes[2]
    lengths = tuple(c * s * CELL for c, s in zip(cells, sizes))
    length_x, length_y, length_z = lengths
    screen = 2 * cells_y * CELL
    pairs = slot_count * NBR

    share = length_z // 2 // devices
    planes = 2 * share
    win_x = -(-(cells_x * CELL + 4) // 16) * 16
    win_y = cells_y * CELL + 8
    assert 2 * cells_z * slot_count == LANES and cells_y % 2 == 0
    assert LANES % (4 * win_x) == 0 and cells_z * CELL + 4 <= LANES
    all_modes = np.arange(length_z // 2)
    table_k = np.stack([all_modes, all_modes], axis=1)
    phase_c = np.stack([np.ones_like(all_modes), np.zeros_like(all_modes)], axis=1)
    table_k[0, 1] = length_z // 2
    phase_c[0, 1] = 1
    table_k = table_k.reshape(devices, planes)
    phase_c = phase_c.reshape(devices, planes).astype(np.float64)
    basis_x, modes_x = trig_basis(length_x)
    basis_y, modes_y = trig_basis(length_y)
    qx, sx = axis_terms(modes_x, length_x)
    qy, sy = axis_terms(modes_y, length_y)
    qz, sz = axis_terms(table_k, length_z)
    krow = np.stack([qy, sy], axis=1).astype(np.float32)
    zrow = np.stack([table_k, phase_c, 1.0 - phase_c, qz, sz], axis=2)
    plane_rows = -(-planes // 8) * 8
    zrow = np.concatenate([zrow, np.ones((devices, plane_rows - planes, 5))], axis=1)
    zrow = zrow.astype(np.float32)
    kx = np.stack([qx, sx]).astype(np.float32)
    grid_x, grid_y = cells_x * CELL, cells_y * CELL
    row_y = np.arange(win_y)
    row_y = np.where(row_y < grid_y + 4, row_y, row_y - 4)
    at_y = np.concatenate([(row_y + g * grid_y - 1) % length_y for g in range(sizes[1])])
    by = basis_y[:, at_y]
    per_block = LANES // (2 * win_x)
    blocks = -(-sizes[0] // per_block)
    forward = np.zeros((blocks, LANES, length_x))
    backward = np.zeros((length_x, sizes[0] * LANES))
    for g in range(sizes[0]):
        cols = basis_x[:, (np.arange(win_x) + g * grid_x - 1) % length_x]
        at = g % per_block * 2 * win_x
        forward[g // per_block, at : at + 2 * win_x] = np.concatenate([cols, cols], axis=1).T
        backward[:, g * LANES : g * LANES + 4 * win_x] = np.concatenate([cols] * 4, axis=1)
    tables = [jnp.asarray(zrow), jnp.asarray(krow), jnp.asarray(kx)]
    by_hi, by_lo = host_pieces(by)
    tables.append(np.stack([by_hi, by_lo]))
    tables.append(np.concatenate([by_hi.T, by_hi.T, by_lo.T], axis=1))
    for table in (forward, backward):
        tables += host_pieces(table)
    tables = [jnp.asarray(t) for t in tables]

    operands = (
        features,
        features.reshape(atom_count, channels),
        positions.reshape(cell_count, 3 * slot_count),
        species.reshape(cell_count, slot_count),
        neighbours.reshape(cell_count, pairs),
        neighbour_count.reshape(cell_count, slot_count),
        w_self,
        w_neighbour,
        w_radial,
        radial_rates,
        w_pair1,
        w_pair2,
        w_vector,
        w_out,
        w_charge,
        species_charge,
        *tables,
    )
    vmem = pl.BlockSpec(memory_space=pltpu.VMEM)
    dma = pltpu.SemaphoreType.DMA
    groups = sizes[0] * sizes[1]
    lanes = sizes[2] * atom_count
    columns = (cells_x + 2) * (cells_y + 2)
    updated, site_potential = pl.pallas_call(
        functools.partial(
            staged_kernel, sizes, cells, lengths, screen, planes, win_x, win_y, len(operands)
        ),
        out_shape=(
            jax.ShapeDtypeStruct((atom_count, channels), bf16),
            jax.ShapeDtypeStruct((cell_count, slot_count), f32),
        ),
        in_specs=[pl.BlockSpec(memory_space=pl.ANY)] * len(operands),
        out_specs=(vmem, vmem),
        scratch_shapes=[
            pltpu.VMEM((4, atom_count), f32),
            pltpu.VMEM((devices, 4, atom_count), f32),
            pltpu.VMEM(tuple(c + 2 for c in cells) + (slot_count, channels), bf16),
            pltpu.VMEM((columns, (cells_z + 2) * slot_count, channels), f32),
            pltpu.VMEM((2, atom_count, channels), f32),
            pltpu.VMEM((cell_count // 8, 8, pairs), f32),
            pltpu.VMEM((cell_count // 8, 8, pairs), i32),
            pltpu.VMEM((cell_count // 8, 8, pairs), i32),
            pltpu.VMEM((cell_count // 8, 8, pairs), f32),
            pltpu.VMEM((planes * length_y, length_x), f32),
            pltpu.VMEM((columns // 2, 8, LANES), f32),
            pltpu.VMEM((cells_x * cells_y, 8, LANES), f32),
            pltpu.VMEM((cell_count, 8, pairs), f32),
            pltpu.VMEM((cell_count, 8, pairs), f32),
            pltpu.VMEM((sizes[2], plane_rows, LANES), f32),
            pltpu.VMEM((blocks, planes, sizes[1] * win_y, LANES), f32),
            pltpu.VMEM((planes * length_y, LANES), f32),
            pltpu.VMEM((sizes[0], planes, sizes[1] * win_y, LANES), f32),
            pltpu.VMEM((groups, plane_rows, lanes), f32),
            pltpu.VMEM((5, 4, lanes), f32),
            pltpu.VMEM((plane_rows, lanes), f32),
            pltpu.VMEM((groups, 2 * win_x, lanes), bf16),
            pltpu.VMEM((groups, win_y, lanes), f32),
            pltpu.VMEM((devices, 1, atom_count), f32),
            pltpu.VMEM((devices, 1, atom_count), f32),
            pltpu.VMEM((atom_count, channels), f32),
            pltpu.VMEM((3, atom_count, channels), f32),
            pltpu.VMEM((2 * channels, 2 * channels), bf16),
            pltpu.VMEM((2 * channels, 2 * channels), bf16),
            dma((devices,)),
            dma((devices,)),
            dma((27,)),
            dma((27,)),
            dma((devices,)),
            dma((devices,)),
            pltpu.SemaphoreType.REGULAR((max(max(size // 2 for size in sizes) - 1, 1),)),
            dma((len(operands),)),
        ]
        + [
            (pltpu.SMEM if a is radial_rates or a is species_charge else pltpu.VMEM)(
                a.shape, a.dtype
            )
            for a in operands
        ],
        name="fused_layer",
        compiler_params=pltpu.CompilerParams(
            has_side_effects=True, collective_id=0, vmem_limit_bytes=VMEM_BYTES
        ),
    )(*operands)
    return (
        updated.reshape(features.shape),
        site_potential.reshape(cells_x, cells_y, cells_z, slot_count),
    )


def solution(mesh):
    cells = P("gx", "gy", "gz", None)
    return jax.shard_map(
        shards,
        mesh=mesh,
        in_specs=(P("gx", "gy", "gz", None, None),) + (cells,) * 5 + (P(),) * 10,
        out_specs=(P("gx", "gy", "gz", None, None), cells),
        check_vma=False,
    )
```
